256 devices in a mesh: gz: 64 (over y, z, core), ga: 4 (over x).
Axes of the slice: x: 4, y: 4, z: 8, core: 2. Of those that a mesh axis runs over, the one named last changes fastest.
Arguments:
- solution: float32 [512, 256, 256], P(('gz', 'ga')), may hold values from -6 to 6
- residual: float32 [512, 256, 256], P(('gz', 'ga')), may hold values from -40 to 40
- direction: float32 [512, 256, 256], P(('gz', 'ga')), may hold values from -40 to 40
Outputs:
- solution_out: float32 [512, 256, 256], P(('gz', 'ga'))
- residual_out: float32 [512, 256, 256], P(('gz', 'ga'))
- direction_out: float32 [512, 256, 256], P(('gz', 'ga'))
The draws below stay inside these ranges and needn't reach their ends.
All inputs are finite; a program needn't handle non-finite values.
Results may differ from the reference program's by a relative error of at most 0.0003.
Values sent between devices are 32-bit elements; how exact they have to be, the bound alone decides.
No kernel may reach another device: no remote copies, remote signals or barrier semaphores. Data moves between devices by JAX's collectives and lax.ppermute only.
A program may use at most 128 MiB of HBM per device.

```python
import math
import jax
import jax.numpy as jnp
import numpy as np
from jax import lax

NX = 256
NY = 256
S = 8
NZ = 512


def base_noise(key):
    return jnp.clip(jax.random.normal(key, (NZ, NX, NY), jnp.float32), -3.0, 3.0)


def box_filter(field):
    padded = jnp.pad(field, ((0, 0), (1, 1), (1, 1)))
    total = jnp.zeros_like(field)
    for shift_x in range(3):
        for shift_y in range(3):
            total = total + padded[:, shift_x:shift_x + NX, shift_y:shift_y + NY]
    return total / 3.0


def checker_sign():
    plane_ids = jnp.arange(NZ, dtype=jnp.int32)[:, None, None]
    column_ids = jnp.arange(NX, dtype=jnp.int32)[None, :, None]
    row_ids = jnp.arange(NY, dtype=jnp.int32)[None, None, :]
    parity = (plane_ids + column_ids + row_ids) % 2
    return 1.0 - 2.0 * parity.astype(jnp.float32)


def block_table(key, low, high, width):
    count = (NZ + width - 1) // width
    plane_ids = jnp.arange(NZ, dtype=jnp.int32)
    values = jax.random.uniform(key, (count,), jnp.float32, low, high)
    return values[plane_ids // width]


def mixed_field(key, salt):
    white = base_noise(jax.random.fold_in(key, salt + 1))
    smooth = box_filter(base_noise(jax.random.fold_in(key, salt + 2)))
    rough = checker_sign() * box_filter(base_noise(jax.random.fold_in(key, salt + 3)))
    mixing = block_table(jax.random.fold_in(key, salt + 4), -1.2, 1.2, 8)
    mixing = mixing + block_table(jax.random.fold_in(key, salt + 5), -0.5, 0.5, 2)
    upward = jnp.maximum(mixing, 0.0)[:, None, None]
    downward = jnp.maximum(-mixing, 0.0)[:, None, None]
    field = white + upward * smooth + downward * rough
    amplitude = jnp.exp(block_table(jax.random.fold_in(key, salt + 6), 0.0, math.log(10.0), 8))
    return (field, amplitude)


def paired_fields(key):
    depth = jnp.arange(NZ, dtype=jnp.float32) / max(NZ - 1, 1)
    direction_base, direction_amp = mixed_field(key, 100)
    residual_base, residual_amp = mixed_field(key, 200)
    coupling = block_table(jax.random.fold_in(key, 301), -1.0, 1.0, 8)
    coupling = coupling + block_table(jax.random.fold_in(key, 302), -0.3, 0.3, 2)
    trend = 3.0 ** depth
    direction = (0.2 * trend * direction_amp)[:, None, None] * direction_base
    residual = (0.2 * trend * residual_amp)[:, None, None] * (residual_base + coupling[:, None, None] * direction_base)
    return (jnp.clip(residual, -39.0, 39.0), jnp.clip(direction, -39.0, 39.0))


def draw_residual(key, part):
    return paired_fields(key)[0]


def draw_direction(key, part):
    return paired_fields(key)[1]


def shard_levels(own_key, dims, pieces, least, largest):
    factor_of = 1.0
    for dim, parts in pieces:
        steps = jax.random.uniform(jax.random.fold_in(jax.random.fold_in(own_key, 6), dim), (parts,), jnp.float32, least / len(pieces), largest / len(pieces))
        factor_of = factor_of * jnp.repeat(jnp.exp(steps), dims[dim] // parts).reshape((-1,) + (1,) * (len(dims) - 1 - dim))
    return factor_of


def scatter_about(stream_key, extent, spread, reach, cuts=(), kind=jnp.bfloat16):
    drawn = spread * jax.random.normal(stream_key, extent, jnp.float32)
    if cuts:
        drawn = drawn * shard_levels(stream_key, extent, cuts, -0.22, 0.18)
    return jnp.clip(drawn, -reach, reach).astype(kind)


def setup_inputs(seed: int = 0) -> dict:
    arg_keys = jax.random.split(jax.random.key(seed), 4)
    solution = scatter_about(arg_keys[0], (NZ, NX, NY), 1.0, 6.0, ((0, 256),), jnp.float32)
    residual = draw_residual(jax.random.fold_in(arg_keys[3], 71), 0)
    direction = draw_direction(jax.random.fold_in(arg_keys[3], 71), 0)
    return dict(solution=solution, residual=residual, direction=direction)


precise = lax.Precision.HIGHEST
first_scale = -1.0 / 6.0
next_scale = -1.0 / 3.0


def neighbours_padded(extended):
    centre = extended[:, 1:-1]
    total = extended[:, 2:] + extended[:, :-2]
    padded = jnp.pad(centre, ((0, 0), (0, 0), (1, 1), (1, 1)))
    total = total + padded[:, :, 2:, 1:-1] + padded[:, :, :-2, 1:-1]
    total = total + padded[:, :, 1:-1, 2:] + padded[:, :, 1:-1, :-2]
    return total


def change_matrix(steps):
    count = 2 * steps + 1
    table = np.zeros((count, count), np.float32)
    for offset, length in ((0, steps + 1), (steps + 1, steps)):
        for power in range(length - 1):
            column = offset + power
            table[column, column] = 6.0
            if power == 0:
                table[column + 1, column] = 6.0
            else:
                table[column + 1, column] = 3.0
                table[column - 1, column] = 3.0
    return table


def quadratic(left, gram, right):
    return jnp.dot(left, jnp.dot(gram, right, precision=precise), precision=precise)


def inner_steps(gram, steps):
    table = jnp.asarray(change_matrix(steps), jnp.float32)
    count = 2 * steps + 1
    unit_rows = jnp.eye(count, dtype=jnp.float32)
    search = unit_rows[0]
    remain = unit_rows[steps + 1]
    iterate = jnp.zeros((count,), jnp.float32)
    current = quadratic(remain, gram, remain)
    for step in range(steps):
        moved = jnp.dot(table, search, precision=precise)
        alpha = current / quadratic(search, gram, moved)
        iterate = iterate + alpha * search
        remain = remain - alpha * moved
        updated = quadratic(remain, gram, remain)
        search = remain + (updated / current) * search
        current = updated
    return jnp.stack([iterate, remain, search])


def reference(solution, residual, direction):
    current = jnp.stack([direction, residual])
    earlier = current
    search_chain = [direction]
    residual_chain = [residual]
    for power in range(1, S + 1):
        active = current if power < S else current[0:1]
        beside = neighbours_padded(jnp.pad(active, ((0, 0), (1, 1), (0, 0), (0, 0))))
        if power == 1:
            following = beside * first_scale
        else:
            following = beside * next_scale - earlier[:active.shape[0]]
        earlier = active
        current = following
        search_chain.append(following[0])
        if power < S:
            residual_chain.append(following[1])
    basis = jnp.stack(search_chain + residual_chain)
    flat = basis.reshape(basis.shape[0], -1)
    gram = jnp.dot(flat, flat.T, precision=precise, preferred_element_type=jnp.float32)
    coefs = inner_steps(gram, S)
    combined = jnp.dot(coefs, flat, precision=precise, preferred_element_type=jnp.float32)
    shape = solution.shape
    return (solution + combined[0].reshape(shape), combined[1].reshape(shape), combined[2].reshape(shape))
```

```python
import functools

import jax
import jax.numpy as jnp
import numpy as np
from jax import lax
from jax.experimental import pallas as pl
from jax.experimental.pallas import tpu as pltpu
from jax.sharding import Mesh, PartitionSpec as P

S = 8
COLS = 2 * S + 1
PLANES = 8
HALO = 8
LANES = 256
TALL = PLANES + 2 * HALO
FIRST = -1.0 / 6.0
NEXT = -1.0 / 3.0
ALL = ("zz", "c", "x")

DD, RR, DR = 0, 2 * S + 1, 4 * S
SUMS = 6 * S


def chain_kernel(place, own, side, across, basis, sums, ext_d, ext_r, parts):
    rows = own.shape[3]
    keep = rows - 2 * HALO
    core, first, last, low_x, high_x = (place[i] for i in range(5))

    row = lax.broadcasted_iota(jnp.int32, (rows, LANES), 0)
    lane = lax.broadcasted_iota(jnp.int32, (rows, LANES), 1)
    inside = jnp.logical_and(
        jnp.logical_or(row >= HALO, low_x == 0), jnp.logical_or(row < rows - HALO, high_x == 0)
    ).astype(jnp.float32)
    left_edge, right_edge = lane == 0, lane == LANES - 1

    def fold(product):
        total = jnp.sum(product.reshape(keep // 8, 8, LANES), axis=0)
        return total[:, :128] + total[:, 128:]

    for field, ext in ((0, ext_d), (1, ext_r)):
        for plane in range(PLANES):
            ext[0, HALO + plane] = own[plane // 2, field, plane % 2]

        @pl.when(core == 0)
        def _():
            for plane in range(PLANES):
                ext[0, plane] = across[plane // 2, field, plane % 2]
                ext[0, HALO + PLANES + plane] = side[plane // 2, field, plane % 2]

        @pl.when(core != 0)
        def _():
            for plane in range(PLANES):
                ext[0, plane] = side[plane // 2, field, plane % 2]
                ext[0, HALO + PLANES + plane] = across[plane // 2, field, plane % 2]

    def stencil(ext, now, plane):
        here = ext[now, plane]
        total = ext[now, plane - 1] + ext[now, plane + 1]
        total = total + pltpu.roll(here, 1, 0) + pltpu.roll(here, rows - 1, 0)
        left = jnp.where(left_edge, 0.0, pltpu.roll(here, 1, 1))
        right = jnp.where(right_edge, 0.0, pltpu.roll(here, LANES - 1, 1))
        return here, total + (left + right)

    def advance(ext, power, column, visit):
        now, new = (power - 1) % 3, power % 3
        old = (power - 2) % 3
        scale = FIRST if power == 1 else NEXT

        def one(plane, factor):
            here, total = stencil(ext, now, plane)
            value = total * factor
            if power > 1:
                value = value - ext[old, plane]
            ext[new, plane] = value
            return here, value

        def outer(factor):
            def body(plane, _):
                one(plane, factor)
                return 0

            return body

        lax.fori_loop(power, HALO, outer(inside * (scale * first)), 0)

        def body(plane, accs):
            here, value = one(HALO + plane, inside * scale)
            here, value = here[HALO : HALO + keep], value[HALO : HALO + keep]
            basis[column, plane] = value
            return visit(accs, plane, here, value)

        accs = lax.fori_loop(0, PLANES, body, tuple(jnp.zeros((8, 128), jnp.float32) for _ in range(visit.count)))
        lax.fori_loop(HALO + PLANES, TALL - power, outer(inside * (scale * last)), 0)
        return accs

    def of_own(accs, plane, here, value):
        return accs[0] + fold(value * value), accs[1] + fold(here * value)

    of_own.count = 2

    def put(index, acc):
        parts[pl.ds(index, 1), :] = jnp.sum(acc, axis=0, keepdims=True)

    parts[...] = jnp.zeros_like(parts)

    def start(plane, accs):
        d = ext_d[0, HALO + plane, HALO : HALO + keep]
        r = ext_r[0, HALO + plane, HALO : HALO + keep]
        basis[0, plane] = d
        basis[S + 1, plane] = r
        return accs[0] + fold(d * d), accs[1] + fold(r * r), accs[2] + fold(d * r)

    zero = jnp.zeros((8, 128), jnp.float32)
    dd, rr, dr = lax.fori_loop(0, PLANES, start, (zero, zero, zero))
    put(DD, dd)
    put(RR, rr)
    put(DR, dr)

    for power in range(1, S + 1):
        same, next_to = advance(ext_d, power, power, of_own)
        put(DD + 2 * power, same)
        put(DD + 2 * power - 1, next_to)

    def ahead(plane, acc):
        return acc + fold(basis[1, plane] * basis[S + 1, plane])

    put(DR + 1, lax.fori_loop(0, PLANES, ahead, zero))

    for power in range(1, S):

        def visit(accs, plane, here, value, power=power):
            return (
                accs[0] + fold(value * value),
                accs[1] + fold(here * value),
                accs[2] + fold(basis[power, plane] * value),
                accs[3] + fold(basis[power + 1, plane] * value),
            )

        visit.count = 4
        same, next_to, cross, cross_next = advance(ext_r, power, S + 1 + power, visit)
        put(RR + 2 * power, same)
        put(RR + 2 * power - 1, next_to)
        put(DR + 2 * power, cross)
        put(DR + 2 * power + 1, cross_next)

    sums[...] = jnp.sum(parts[...].T, axis=0, keepdims=True)


def coefficients(sums):
    tall = 24
    shape = (tall, 128)
    i = lax.broadcasted_iota(jnp.int32, shape, 0)
    j = lax.broadcasted_iota(jnp.int32, shape, 1)
    row_r, col_r = i > S, j > S
    a = jnp.where(row_r, i - (S + 1), i)
    b = jnp.where(col_r, j - (S + 1), j)
    valid = jnp.logical_and(i < COLS, j < COLS)
    base = jnp.where(row_r, jnp.where(col_r, RR, DR), jnp.where(col_r, DR, DD))
    plus = a + b
    minus = jnp.abs(a - b)
    odd = plus & 1
    at_plus = jnp.where(valid, base + plus, -1)
    at_minus = jnp.where(valid, base + minus, -1)
    at_base = jnp.where(valid, base + odd, -1)
    gram = jnp.zeros(shape, jnp.float32)
    for place in range(SUMS):
        weight = (
            (at_plus == place).astype(jnp.float32)
            + (at_minus == place).astype(jnp.float32)
            - (at_base == place).astype(jnp.float32)
        )
        gram = gram + weight * sums[:, place : place + 1]

    def change(index, axis):
        second = index > S
        k = jnp.where(second, index - (S + 1), index)
        count = jnp.where(second, S, S + 1)
        valid = index < COLS
        middle = jnp.where(jnp.logical_and(valid, k < count - 1), 6.0, 0.0)
        below = jnp.where(jnp.logical_and(valid, k >= 1), jnp.where(k == 1, 6.0, 3.0), 0.0)
        above = jnp.where(jnp.logical_and(valid, k + 1 < count - 1), 3.0, 0.0)
        size = shape[axis]

        def apply(v):
            return middle * v + below * pltpu.roll(v, 1, axis) + above * pltpu.roll(v, size - 1, axis)

        return apply

    down, along = change(i, 0), change(j, 1)

    def quadratic(left_down, right_along):
        return jnp.sum(left_down * (gram * right_along), keepdims=True)

    def unit(index, k):
        return (index == k).astype(jnp.float32)

    q_d, q_a = unit(i, 0), unit(j, 0)
    w_d, w_a = unit(i, S + 1), unit(j, S + 1)
    c_d = jnp.zeros(shape, jnp.float32)
    rho = quadratic(w_d, w_a)
    for _ in range(S):
        m_d, m_a = down(q_d), along(q_a)
        alpha = rho / quadratic(q_d, m_a)
        c_d = c_d + alpha * q_d
        w_d, w_a = w_d - alpha * m_d, w_a - alpha * m_a
        rho_new = quadratic(w_d, w_a)
        beta = rho_new / rho
        q_d, q_a = w_d + beta * q_d, w_a + beta * q_a
        rho = rho_new
    return c_d, w_d, q_d


def combine_kernel(sums, basis, out, coefs):
    total = jnp.sum(sums[...], axis=0, keepdims=True)
    for which, value in enumerate(coefficients(total)):
        coefs[which] = value
    keep = basis.shape[2]
    tile = 16
    splat = {}

    def body(step, _):
        plane = step // (keep // tile)
        row = pl.multiple_of((step % (keep // tile)) * tile, tile)
        accs = [None] * 3
        for k in range(COLS):
            v = basis[k, plane, pl.ds(row, tile)]
            for which in range(3):
                factor = coefs[which, k : k + 1, :]
                term = v * jnp.concatenate([factor, factor], axis=1)
                accs[which] = term if accs[which] is None else accs[which] + term
        for which in range(3):
            out[plane // 2, which, plane % 2, pl.ds(row, tile)] = accs[which]
        return 0

    lax.fori_loop(0, PLANES * (keep // tile), body, 0)


def on_device(solution, residual, direction):
    groups = lax.axis_size("x")
    x, c, zz = lax.axis_index("x"), lax.axis_index("c"), lax.axis_index("zz")
    outer = lax.axis_size("zz")
    per, height, lanes = direction.shape
    keep = height // groups
    rows = keep + 2 * HALO

    fields = jnp.pad(jnp.stack([direction, residual]), ((0, 0), (0, 0), (HALO, HALO), (0, 0)))
    pieces = jnp.stack([fields[:, :, g * keep : g * keep + rows] for g in range(groups)])
    own = lax.all_to_all(pieces, "x", 0, 0, tiled=True)

    blocks = 2 * outer
    near = [(b, b - 1) for b in range(0, blocks, 2) if b > 0] + [(b, b + 1) for b in range(1, blocks, 2) if b + 1 < blocks]
    across = lax.ppermute(own, ("zz", "c"), near)
    side = lax.ppermute(own, "c", [(0, 1), (1, 0)])

    place = jnp.stack(
        [
            c,
            1 - jnp.logical_and(zz == 0, c == 0).astype(jnp.int32),
            1 - jnp.logical_and(zz == outer - 1, c == 1).astype(jnp.int32),
            (x == 0).astype(jnp.int32),
            (x == groups - 1).astype(jnp.int32),
        ]
    ).astype(jnp.int32)

    vmem = pl.BlockSpec(memory_space=pltpu.VMEM)
    basis, sums = pl.pallas_call(
        chain_kernel,
        out_shape=(
            jax.ShapeDtypeStruct((COLS, PLANES, keep, lanes), jnp.float32),
            jax.ShapeDtypeStruct((1, 128), jnp.float32),
        ),
        in_specs=[pl.BlockSpec(memory_space=pltpu.SMEM), vmem, vmem, vmem],
        out_specs=(vmem, vmem),
        scratch_shapes=[
            pltpu.VMEM((3, TALL, rows, lanes), jnp.float32),
            pltpu.VMEM((3, TALL, rows, lanes), jnp.float32),
            pltpu.VMEM((128, 128), jnp.float32),
        ],
        compiler_params=pltpu.CompilerParams(vmem_limit_bytes=40 * 2**20),
        name="chains",
    )(place, own, side, across)

    devices = groups * blocks
    everyone = lax.all_to_all(jnp.broadcast_to(sums[None], (devices, 1, 128)), ALL, 0, 0, tiled=True)

    mixed = pl.pallas_call(
        combine_kernel,
        out_shape=jax.ShapeDtypeStruct((groups, 3, per, keep, lanes), jnp.float32),
        in_specs=[vmem, vmem],
        out_specs=vmem,
        scratch_shapes=[pltpu.VMEM((3, 24, 128), jnp.float32)],
        compiler_params=pltpu.CompilerParams(vmem_limit_bytes=20 * 2**20),
        name="combine",
    )(everyone.reshape(devices, 128), basis)

    back = lax.all_to_all(mixed, "x", 0, 0, tiled=True)
    whole = [jnp.swapaxes(back[:, which], 0, 1).reshape(per, height, lanes) for which in range(3)]
    return solution + whole[0], whole[1], whole[2]


def solution(mesh):
    blocks, groups = mesh.devices.shape
    split = Mesh(mesh.devices.reshape(blocks // 2, 2, groups), ALL)
    spec = P(ALL, None, None)
    return jax.shard_map(
        on_device, mesh=split, in_specs=(spec, spec, spec), out_specs=(spec, spec, spec), check_vma=False
    )
```

```python
import functools

import jax
import jax.numpy as jnp
import numpy as np
from jax import lax
from jax.experimental import pallas as pl
from jax.experimental.pallas import tpu as pltpu
from jax.sharding import Mesh, PartitionSpec as P

S = 8
COLS = 2 * S + 1
PLANES = 8
HALO = 8
PAD = 8
HALF = 128
GROUP = 4
FIRST = -1.0 / 6.0
NEXT = -1.0 / 3.0
ALL = ("zz", "c", "x")
VMEM = pl.BlockSpec(memory_space=pltpu.VMEM)
SMEM = pl.BlockSpec(memory_space=pltpu.SMEM)
HBM = pl.BlockSpec(memory_space=pltpu.HBM)

DD, RR, DR = 0, 2 * S + 1, 4 * S
SUMS = 6 * S


def chain_plan(steps):
    lows = [HALO - steps + k for k in range(steps + 1)]
    groups = [0] + [-(-(PLANES + 2 * (steps - k)) // GROUP) for k in range(1, steps + 1)]
    held = []
    for k in range(steps + 1):
        own = GROUP * groups[k] if k else PLANES + 2 * steps
        read = GROUP * groups[k + 1] + 2 if k < steps else 0
        held.append(max(own, read))
    return lows, groups, held


def pack_kernel(direction, residual, out_d, out_r, sem):
    pieces, per, halves, rows, _ = out_d.shape
    height = direction.shape[1]
    keep = rows - 2 * HALO
    copies = []
    for source, out in ((direction, out_d), (residual, out_r)):
        for g in range(pieces):
            low = max(g * keep - HALO, 0)
            high = min((g + 1) * keep + HALO, height)
            at = low - (g * keep - HALO)
            for h in range(halves):
                copies.append(
                    pltpu.make_async_copy(
                        source.at[:, pl.ds(low, high - low), pl.ds(h * HALF, HALF)],
                        out.at[g, :, h, pl.ds(at, high - low), :],
                        sem.at[len(copies)],
                    )
                )
    for copy in copies:
        copy.start()
    for out in (out_d, out_r):
        zeros = jnp.zeros((per, halves, HALO, HALF), jnp.float32)
        out[0, :, :, :HALO] = zeros
        out[pieces - 1, :, :, rows - HALO :] = zeros
    for copy in copies:
        copy.wait()


def run_chain(place, own, side, across, chain, sideways, steps):
    lows, groups, _ = chain_plan(steps)
    rows = own.shape[3]
    core = place[0]
    data = pl.ds(PAD, rows)

    def load(target, source, plane):
        for h in range(2):
            chain[0][target - lows[0], h, data] = source[plane // 2, plane % 2, h]

    for plane in range(PLANES):
        load(HALO + plane, own, plane)

    def halo(low, high):
        for plane in range(PLANES - steps, PLANES):
            load(plane, low, plane)
        for plane in range(steps):
            load(HALO + PLANES + plane, high, plane)

    @pl.when(core == 0)
    def _():
        halo(across, side)

    @pl.when(core != 0)
    def _():
        halo(side, across)

    lane = lax.broadcasted_iota(jnp.int32, (rows, HALF), 1)
    at_low, at_high = lane == 0, lane == HALF - 1

    def neighbours_y(power, plane, u):
        source = chain[power - 1]
        index = plane + u - lows[power - 1]
        a, b = source[index, 0, data], source[index, 1, data]
        up_a, up_b = pltpu.roll(a, 1, 1), pltpu.roll(b, 1, 1)
        down_a, down_b = pltpu.roll(a, HALF - 1, 1), pltpu.roll(b, HALF - 1, 1)
        first = jnp.where(at_low, 0.0, up_a) + jnp.where(at_high, down_b, down_a)
        second = jnp.where(at_low, up_a, up_b) + jnp.where(at_high, 0.0, down_b)
        return first, second

    low_valid, high_valid, low_x, high_x = (place[i].astype(jnp.float32) for i in range(1, 5))

    def values(power, plane, u):
        now, new = chain[power - 1], chain[power]
        index = plane + u - lows[power - 1]
        where = plane + u
        scale = FIRST if power == 1 else NEXT
        outside_low = jnp.logical_and(where < HALO, place[1] == 0)
        outside_high = jnp.logical_and(where >= HALO + PLANES, place[2] == 0)
        scale = jnp.where(jnp.logical_or(outside_low, outside_high), 0.0, scale)
        for h in range(2):
            total = now[index - 1, h, data] + now[index + 1, h, data]
            total = total + (now[index, h, pl.ds(PAD - 1, rows)] + now[index, h, pl.ds(PAD + 1, rows)])
            total = total + sideways[u, h]
            parts = []
            for a, b, weight in ((0, HALO, low_x), (HALO, rows - HALO, None), (rows - HALO, rows, high_x)):
                factor = scale if weight is None else scale * weight
                parts.append(total[a:b] * factor)
            value = jnp.concatenate(parts, axis=0)
            if power > 1:
                value = value - chain[power - 2][plane + u - lows[power - 2], h, data]
            new[plane + u - lows[power], h, data] = value

    def group(power, plane, then):
        ahead = [neighbours_y(*then, u) for u in range(GROUP)] if then else []
        for u in range(GROUP):
            values(power, plane, u)
        for u, pair in enumerate(ahead):
            sideways[u, 0], sideways[u, 1] = pair

    for u in range(GROUP):
        sideways[u, 0], sideways[u, 1] = neighbours_y(1, lows[1], u)
    for power in range(1, steps + 1):

        def body(g, _, power=power):
            plane = lows[power] + GROUP * g
            group(power, plane, (power, plane + GROUP))
            return 0

        lax.fori_loop(0, groups[power] - 1, body, 0)
        last = lows[power] + GROUP * (groups[power] - 1)
        group(power, last, (power + 1, lows[power + 1]) if power < steps else None)


def own_of(chain, steps, k, plane, h, row):
    low = chain_plan(steps)[0][k]
    return chain[k][HALO + plane - low, h, pl.ds(row, 8)]


def products(count, keep, terms):
    def body(step, accs):
        plane, tile = step // (keep // 8), step % (keep // 8)
        row = pl.multiple_of(PAD + HALO + 8 * tile, 8)
        for h in range(2):
            accs = tuple(acc + x * y for acc, (x, y) in zip(accs, terms(plane, h, row)))
        return accs

    zero = jnp.zeros((8, HALF), jnp.float32)
    return lax.fori_loop(0, PLANES * (keep // 8), body, (zero,) * count)


def chain_terms(values):
    terms = [(values[0], values[0])]
    for k in range(1, len(values)):
        terms += [(values[k - 1], values[k]), (values[k], values[k])]
    return terms


def direction_kernel(place, own, side, across, *refs):
    chain, parts, sideways = refs[: S + 1], refs[S + 1], refs[S + 2]
    run_chain(place, own, side, across, chain, sideways, S)
    keep = own.shape[3] - 2 * HALO
    sums = products(
        2 * S + 1,
        keep,
        lambda plane, h, row: chain_terms([own_of(chain, S, k, plane, h, row) for k in range(S + 1)]),
    )
    parts[...] = jnp.zeros_like(parts)
    for k, total in enumerate(sums):
        parts[pl.ds(DD + k, 1), :] = jnp.sum(total, axis=0, keepdims=True)


def residual_kernel(place, own, side, across, *refs):
    other, parts_d, chain, sums, sideways, parts = (
        refs[: S + 1],
        refs[S + 1],
        refs[S + 2 : 2 * S + 2],
        refs[2 * S + 2],
        refs[2 * S + 3],
        refs[2 * S + 4],
    )
    run_chain(place, own, side, across, chain, sideways, S - 1)
    keep = own.shape[3] - 2 * HALO
    parts[...] = parts_d[...]

    def put(index, total):
        parts[pl.ds(index, 1), :] = jnp.sum(total, axis=0, keepdims=True)

    of_r = products(
        2 * S - 1,
        keep,
        lambda plane, h, row: chain_terms([own_of(chain, S - 1, k, plane, h, row) for k in range(S)]),
    )
    for k, total in enumerate(of_r):
        put(RR + k, total)

    def cross(plane, h, row):
        d = [own_of(other, S, k, plane, h, row) for k in range(S + 1)]
        r = [own_of(chain, S - 1, k, plane, h, row) for k in range(S)]
        terms = []
        for k in range(S):
            terms += [(d[k], r[k]), (d[k + 1], r[k])]
        return terms

    for k, total in enumerate(products(2 * S, keep, cross)):
        put(DR + k, total)
    sums[...] = jnp.sum(parts[...].T, axis=0, keepdims=True)


def coefficients(sums):
    tall = 24
    shape = (tall, 128)
    i = lax.broadcasted_iota(jnp.int32, shape, 0)
    j = lax.broadcasted_iota(jnp.int32, shape, 1)
    row_r, col_r = i > S, j > S
    a = jnp.where(row_r, i - (S + 1), i)
    b = jnp.where(col_r, j - (S + 1), j)
    valid = jnp.logical_and(i < COLS, j < COLS)
    base = jnp.where(row_r, jnp.where(col_r, RR, DR), jnp.where(col_r, DR, DD))
    at_plus = jnp.where(valid, base + a + b, -1)
    at_minus = jnp.where(valid, base + jnp.abs(a - b), -1)
    at_base = jnp.where(valid, base + ((a + b) & 1), -1)
    gram = jnp.zeros(shape, jnp.float32)
    for place in range(SUMS):
        weight = (
            (at_plus == place).astype(jnp.float32)
            + (at_minus == place).astype(jnp.float32)
            - (at_base == place).astype(jnp.float32)
        )
        gram = gram + weight * sums[:, place : place + 1]

    def change(index, axis):
        second = index > S
        k = jnp.where(second, index - (S + 1), index)
        count = jnp.where(second, S, S + 1)
        valid = index < COLS
        middle = jnp.where(jnp.logical_and(valid, k < count - 1), 6.0, 0.0)
        below = jnp.where(jnp.logical_and(valid, k >= 1), jnp.where(k == 1, 6.0, 3.0), 0.0)
        above = jnp.where(jnp.logical_and(valid, k + 1 < count - 1), 3.0, 0.0)
        size = shape[axis]

        def apply(v):
            return middle * v + below * pltpu.roll(v, 1, axis) + above * pltpu.roll(v, size - 1, axis)

        return apply

    down, along = change(i, 0), change(j, 1)

    def quadratic(left_down, right_along):
        return jnp.sum(left_down * (gram * right_along), keepdims=True)

    def unit(index, k):
        return (index == k).astype(jnp.float32)

    q_d, q_a = unit(i, 0), unit(j, 0)
    w_d, w_a = unit(i, S + 1), unit(j, S + 1)
    c_d = jnp.zeros(shape, jnp.float32)
    rho = quadratic(w_d, w_a)
    for _ in range(S):
        m_d, m_a = down(q_d), along(q_a)
        alpha = rho / quadratic(q_d, m_a)
        c_d = c_d + alpha * q_d
        w_d, w_a = w_d - alpha * m_d, w_a - alpha * m_a
        rho_new = quadratic(w_d, w_a)
        beta = rho_new / rho
        q_d, q_a = w_d + beta * q_d, w_a + beta * q_a
        rho = rho_new
    return c_d, w_d, q_d


def combine_kernel(sums, *refs):
    chain_d, chain_r, out, coefs = refs[: S + 1], refs[S + 1 : COLS], refs[COLS], refs[COLS + 1]
    total = jnp.sum(sums[...], axis=0, keepdims=True)
    for which, value in enumerate(coefficients(total)):
        coefs[which] = value
    keep = out.shape[4]
    tile = 16

    def body(step, _):
        plane, at = step // (keep // tile), step % (keep // tile)
        row = pl.multiple_of(at * tile, tile)
        source = pl.ds(pl.multiple_of(PAD + HALO + row, 8), tile)
        sums = [[None] * 3, [None] * 3]
        for k in range(COLS):
            chain, power, steps = (chain_d, k, S) if k <= S else (chain_r, k - S - 1, S - 1)
            low = chain_plan(steps)[0][power]
            factors = [coefs[which, k : k + 1, :] for which in range(3)]
            for h in range(2):
                v = chain[power][HALO + plane - low, h, source]
                for which in range(3):
                    term = v * factors[which]
                    sums[h][which] = term if k == 0 else sums[h][which] + term
        for h in range(2):
            for which in range(3):
                out[plane // 2, which, plane % 2, h, pl.ds(row, tile)] = sums[h][which]
        return 0

    lax.fori_loop(0, PLANES * (keep // tile), body, 0)


def finish_kernel(solution, back, out_x, out_r, out_d, hold, sem):
    pieces, _, per, halves, keep, _ = back.shape
    copies = []
    for which, out in ((1, out_r), (2, out_d), (0, out_x)):
        for g in range(pieces):
            for h in range(halves):
                for plane in range(per):
                    value = back[g, which, plane, h]
                    where = (plane, pl.ds(g * keep, keep), pl.ds(h * HALF, HALF))
                    if which == 0:
                        value = value + solution[where]
                    hold[(which, *where)] = value
        copies.append(pltpu.make_async_copy(hold.at[which], out, sem.at[which]))
        copies[-1].start()
    for copy in copies:
        copy.wait()


def on_device(solution, residual, direction):
    groups = lax.axis_size("x")
    x, c, zz = lax.axis_index("x"), lax.axis_index("c"), lax.axis_index("zz")
    outer = lax.axis_size("zz")
    per, height, lanes = direction.shape
    keep = height // groups
    rows = keep + 2 * HALO
    f32 = jnp.float32

    piece = jax.ShapeDtypeStruct((groups, per, 2, rows, HALF), f32)
    pieces = pl.pallas_call(
        pack_kernel,
        out_shape=(piece, piece),
        in_specs=[HBM, HBM],
        out_specs=(VMEM, VMEM),
        scratch_shapes=[pltpu.SemaphoreType.DMA((4 * groups,))],
        compiler_params=pltpu.CompilerParams(vmem_limit_bytes=8 * 2**20),
        name="pack",
    )(direction, residual)

    blocks = 2 * outer
    near = [(b, b - 1) for b in range(0, blocks, 2) if b > 0] + [(b, b + 1) for b in range(1, blocks, 2) if b + 1 < blocks]
    place = jnp.stack(
        [
            c,
            1 - jnp.logical_and(zz == 0, c == 0).astype(jnp.int32),
            1 - jnp.logical_and(zz == outer - 1, c == 1).astype(jnp.int32),
            (x != 0).astype(jnp.int32),
            (x != groups - 1).astype(jnp.int32),
        ]
    ).astype(jnp.int32)

    def spread(piece):
        own = lax.all_to_all(piece, "x", 0, 0, tiled=True)
        across = lax.ppermute(own, ("zz", "c"), near)
        side = lax.ppermute(own, "c", [(0, 1), (1, 0)])
        return own, side, across

    def chain_shapes(steps):
        return [jax.ShapeDtypeStruct((held, 2, rows + 2 * PAD, HALF), f32) for held in chain_plan(steps)[2]]

    around_d = spread(pieces[0])
    around_r = spread(pieces[1])
    sideways = pltpu.VMEM((GROUP, 2, rows, HALF), f32)
    shapes_d, shapes_r = chain_shapes(S), chain_shapes(S - 1)
    *chain_d, parts = pl.pallas_call(
        direction_kernel,
        out_shape=(*shapes_d, jax.ShapeDtypeStruct((128, 128), f32)),
        in_specs=[SMEM] + [VMEM] * 3,
        out_specs=(VMEM,) * (S + 2),
        scratch_shapes=[sideways],
        compiler_params=pltpu.CompilerParams(vmem_limit_bytes=4 * 2**20),
        cost_estimate=pl.CostEstimate(flops=10**8, bytes_accessed=10**6, transcendentals=0),
        name="direction_chain",
    )(place, *around_d)
    *chain_r, sums = pl.pallas_call(
        residual_kernel,
        out_shape=(*shapes_r, jax.ShapeDtypeStruct((1, 128), f32)),
        in_specs=[SMEM] + [VMEM] * (3 + S + 2),
        out_specs=(VMEM,) * (S + 1),
        scratch_shapes=[sideways, pltpu.VMEM((128, 128), f32)],
        compiler_params=pltpu.CompilerParams(vmem_limit_bytes=4 * 2**20),
        cost_estimate=pl.CostEstimate(flops=10**8, bytes_accessed=10**6, transcendentals=0),
        name="residual_chain",
    )(place, *around_r, *chain_d, parts)

    devices = groups * blocks
    everyone = lax.all_to_all(jnp.broadcast_to(sums[None], (devices, 1, 128)), ALL, 0, 0, tiled=True)

    mixed = pl.pallas_call(
        combine_kernel,
        out_shape=jax.ShapeDtypeStruct((groups, 3, per, 2, keep, HALF), f32),
        in_specs=[VMEM] * (COLS + 1),
        out_specs=VMEM,
        scratch_shapes=[pltpu.VMEM((3, 24, 128), f32)],
        compiler_params=pltpu.CompilerParams(vmem_limit_bytes=4 * 2**20),
        name="combine",
    )(everyone.reshape(devices, 128), *chain_d, *chain_r)

    back = lax.all_to_all(mixed, "x", 0, 0, tiled=True)
    whole = jax.ShapeDtypeStruct((per, height, lanes), f32)
    return pl.pallas_call(
        finish_kernel,
        out_shape=(whole,) * 3,
        in_specs=[VMEM, VMEM],
        out_specs=(HBM,) * 3,
        scratch_shapes=[pltpu.VMEM((3, per, height, lanes), f32), pltpu.SemaphoreType.DMA((3,))],
        compiler_params=pltpu.CompilerParams(vmem_limit_bytes=8 * 2**20),
        name="finish",
    )(solution, back)


def solution(mesh):
    blocks, groups = mesh.devices.shape
    split = Mesh(mesh.devices.reshape(blocks // 2, 2, groups), ALL)
    spec = P(ALL, None, None)
    return jax.shard_map(
        on_device, mesh=split, in_specs=(spec, spec, spec), out_specs=(spec, spec, spec), check_vma=False
    )
```

```python
import functools

import jax
import jax.numpy as jnp
import numpy as np
from jax import lax
from jax.experimental import pallas as pl
from jax.experimental.pallas import tpu as pltpu
from jax.sharding import Mesh, PartitionSpec as P

S = 8
PIECES = 4
COLS = 2 * S + 1
PLANES = 8
HALO = 8
TALL = PLANES + 2 * HALO
PAD = 8
HALF = 128
GROUP = 4
FIRST = -1.0 / 6.0
NEXT = -1.0 / 3.0
ALL = ("zz", "c", "x")
VMEM = pl.BlockSpec(memory_space=pltpu.VMEM)
HBM = pl.BlockSpec(memory_space=pltpu.HBM)

DD, RR, DR = 0, 2 * S + 1, 4 * S
SUMS = 6 * S


def here():
    return lax.axis_index("c"), lax.axis_index("x")


def piece_of(k):
    return (lax.axis_index("x") + k) % PIECES


def chain_plan(steps):
    lows = [0] + [HALO - steps + k for k in range(1, steps + 1)]
    ends = [TALL] + [HALO + PLANES + steps - k for k in range(1, steps + 1)]
    return lows, ends


def pack_kernel(source, *refs):
    outs = refs[-PIECES:]
    per, halves, rows, _ = outs[0].shape
    keep, height = rows - 2 * HALO, source.shape[1]
    for k in range(PIECES):
        g = piece_of(k)
        row = pl.multiple_of(g * keep, keep)
        below = pl.multiple_of(jnp.maximum(row - HALO, 0), HALO)
        above = pl.multiple_of(jnp.minimum(row + keep, height - HALO), HALO)
        has_below, has_above = (g != 0).astype(jnp.float32), (g != PIECES - 1).astype(jnp.float32)
        for plane in range(per):
            for h in range(halves):
                lanes = pl.ds(h * HALF, HALF)
                outs[k][plane, h, :HALO] = source[plane, pl.ds(below, HALO), lanes] * has_below
                outs[k][plane, h, pl.ds(HALO, keep)] = source[plane, pl.ds(row, keep), lanes]
                outs[k][plane, h, rows - HALO :] = source[plane, pl.ds(above, HALO), lanes] * has_above


def join_kernel(*refs):
    for k in range(PIECES):
        refs[PIECES][k] = refs[k][...]


def load_planes(chain, first, source):
    per, rows = source.shape[1], source.shape[3]
    core, _ = here()
    for k in range(PIECES):
        plane = per * piece_of(PIECES - k)
        for p in range(per):
            at = first + jnp.where(core == 0, plane + p, PLANES - 1 - plane - p)
            for h in range(2):
                chain[0][at, h, pl.ds(PAD, rows)] = source[k, p, h]


def run_groups(groups, chain, sideways, rows, steps):
    lows, _ = chain_plan(steps)
    data = pl.ds(PAD, rows)
    core, x = here()
    zz = lax.axis_index("zz")
    last = lax.axis_size("zz") - 1
    alone = jnp.logical_or(jnp.logical_and(zz == 0, core == 0), jnp.logical_and(zz == last, core == 1))
    low_x = (x != 0).astype(jnp.float32)
    high_x = (x != PIECES - 1).astype(jnp.float32)
    across_valid = 1.0 - alone.astype(jnp.float32)
    lane = lax.broadcasted_iota(jnp.int32, (rows, HALF), 1)
    at_low, at_high = lane == 0, lane == HALF - 1

    def neighbours_y(power, plane):
        source = chain[power - 1]
        index = plane - lows[power - 1]
        a, b = source[index, 0, data], source[index, 1, data]
        up_a, up_b = pltpu.roll(a, 1, 1), pltpu.roll(b, 1, 1)
        down_a, down_b = pltpu.roll(a, HALF - 1, 1), pltpu.roll(b, HALF - 1, 1)
        first = jnp.where(at_low, 0.0, up_a) + jnp.where(at_high, down_b, down_a)
        second = jnp.where(at_low, up_a, up_b) + jnp.where(at_high, 0.0, down_b)
        return first, second

    def value(power, plane, slot, across):
        now, new = chain[power - 1], chain[power]
        index = plane - lows[power - 1]
        scale = FIRST if power == 1 else NEXT
        if across:
            scale = scale * across_valid
        for h in range(2):
            total = now[index - 1, h, data] + now[index + 1, h, data]
            total = total + (now[index, h, pl.ds(PAD - 1, rows)] + now[index, h, pl.ds(PAD + 1, rows)])
            total = total + sideways[slot, h]
            parts = []
            for a, b, weight in ((0, HALO, low_x), (HALO, rows - HALO, None), (rows - HALO, rows, high_x)):
                parts.append(total[a:b] * (scale if weight is None else scale * weight))
            result = jnp.concatenate(parts, axis=0)
            if power > 1:
                result = result - chain[power - 2][plane - lows[power - 2], h, data]
            new[plane - lows[power], h, data] = result

    def step(group, then):
        power, plane, count = group
        made = [(power, plane + u) for u in range(count)] if isinstance(plane, int) else []
        ahead, late = [], []
        if then:
            for u in range(then[2]):
                if (then[0] - 1, then[1] + u) in made:
                    late.append(u)
                else:
                    ahead.append((u, neighbours_y(then[0], then[1] + u)))
        for u in range(count):
            value(power, plane + u, u, isinstance(plane, int) and plane + u < HALO)
        ahead += [(u, neighbours_y(then[0], then[1] + u)) for u in late]
        for u, pair in ahead:
            sideways[u, 0], sideways[u, 1] = pair

    first = groups[0]
    for u in range(first[2]):
        sideways[u, 0], sideways[u, 1] = neighbours_y(first[0], first[1] + u)
    at = 0
    while at < len(groups):
        power, plane, count = groups[at]
        run = 0
        while at + run + 1 < len(groups) and groups[at + run + 1] == (power, plane + GROUP * (run + 1), count) and count == GROUP:
            run += 1
        if run >= 2:

            def body(g, _, power=power, plane=plane):
                now = plane + GROUP * g
                step((power, now, GROUP), (power, now + GROUP, GROUP))
                return 0

            lax.fori_loop(0, run, body, 0)
            at += run
        step(groups[at], groups[at + 1] if at + 1 < len(groups) else None)
        at += 1


def near_groups(steps):
    _, ends = chain_plan(steps)
    groups = []
    for power in range(1, steps + 1):
        low, end = HALO + power, ends[power]
        left = end - low
        while left > 0:
            count = min(GROUP, left)
            if left in (5, 6):
                count = 3
            groups.append((power, low, count))
            low, left = low + count, left - count
    return groups


def far_groups(steps):
    lows, _ = chain_plan(steps)
    groups = []
    for power in range(1, steps + 1):
        middle = HALO + power - GROUP
        groups.append((power, middle, GROUP))
        groups.append((power, lows[power], middle - lows[power]))
    return groups


def near_kernel(steps, own, side, *refs):
    chain, sideways = refs[: steps + 1], refs[steps + 1]
    load_planes(chain, HALO, own)
    load_planes(chain, HALO + PLANES, side)
    run_groups(near_groups(steps), chain, sideways, own.shape[3], steps)


def add_products(acc, chain, steps, other, keep):
    lows, _ = chain_plan(steps)
    rows = pl.ds(PAD + HALO, keep)
    acc[...] = jnp.zeros_like(acc)

    def total(a, b):
        return jnp.sum((a * b).reshape(keep // 8, 8, HALF), axis=0)

    def body(step, _):
        plane, h = step // 2, step % 2

        def of(chain, steps, k):
            return chain[k][HALO + plane - chain_plan(steps)[0][k], h, rows]

        before, beside = None, None
        if other:
            beside = of(other, S, 0)
        for k in range(steps + 1):
            now = of(chain, steps, k)
            acc[2 * k] += total(now, now)
            if k:
                acc[2 * k - 1] += total(before, now)
            if other:
                following = of(other, S, k + 1)
                acc[2 * steps + 1 + 2 * k] += total(beside, now)
                acc[2 * steps + 2 + 2 * k] += total(following, now)
                beside = following
            before = now
        return 0

    lax.fori_loop(0, 2 * PLANES, body, 0)


def put_products(acc, parts, place):
    for k in range(acc.shape[0]):
        parts[pl.ds(place + k, 1), :] = jnp.sum(acc[k], axis=0, keepdims=True)


def far_direction_kernel(across, *refs):
    chain, parts, sideways, acc = refs[S + 1 : 2 * S + 2], refs[2 * S + 2], refs[2 * S + 3], refs[2 * S + 4]
    rows = across.shape[3]
    load_planes(chain, 0, across)
    run_groups(far_groups(S), chain, sideways, rows, S)
    add_products(acc, chain, S, None, rows - 2 * HALO)
    parts[...] = jnp.zeros_like(parts)
    put_products(acc, parts, DD)


def far_residual_kernel(across, *refs):
    other, parts_d, refs = refs[: S + 1], refs[S + 1], refs[S + 2 :]
    chain, sums, sideways, acc, parts = refs[S : 2 * S], refs[2 * S], refs[2 * S + 1], refs[2 * S + 2], refs[2 * S + 3]
    rows = across.shape[3]
    load_planes(chain, 0, across)
    run_groups(far_groups(S - 1), chain, sideways, rows, S - 1)
    add_products(acc, chain, S - 1, other, rows - 2 * HALO)
    parts[...] = parts_d[...]
    put_products(acc, parts, RR)
    sums[...] = jnp.sum(parts[...].T, axis=0, keepdims=True)


def coefficients(sums):
    tall = 24
    shape = (tall, 128)
    i = lax.broadcasted_iota(jnp.int32, shape, 0)
    j = lax.broadcasted_iota(jnp.int32, shape, 1)
    row_r, col_r = i > S, j > S
    a = jnp.where(row_r, i - (S + 1), i)
    b = jnp.where(col_r, j - (S + 1), j)
    valid = jnp.logical_and(i < COLS, j < COLS)
    base = jnp.where(row_r, jnp.where(col_r, RR, DR), jnp.where(col_r, DR, DD))
    at_plus = jnp.where(valid, base + a + b, -1)
    at_minus = jnp.where(valid, base + jnp.abs(a - b), -1)
    at_base = jnp.where(valid, base + ((a + b) & 1), -1)
    gram = jnp.zeros(shape, jnp.float32)
    for place in range(SUMS):
        weight = (
            (at_plus == place).astype(jnp.float32)
            + (at_minus == place).astype(jnp.float32)
            - (at_base == place).astype(jnp.float32)
        )
        gram = gram + weight * sums[:, place : place + 1]

    def change(index, axis):
        second = index > S
        k = jnp.where(second, index - (S + 1), index)
        count = jnp.where(second, S, S + 1)
        valid = index < COLS
        middle = jnp.where(jnp.logical_and(valid, k < count - 1), 6.0, 0.0)
        below = jnp.where(jnp.logical_and(valid, k >= 1), jnp.where(k == 1, 6.0, 3.0), 0.0)
        above = jnp.where(jnp.logical_and(valid, k + 1 < count - 1), 3.0, 0.0)
        size = shape[axis]

        def apply(v):
            return middle * v + below * pltpu.roll(v, 1, axis) + above * pltpu.roll(v, size - 1, axis)

        return apply

    down, along = change(i, 0), change(j, 1)

    def quadratic(left_down, right_along):
        return jnp.sum(left_down * (gram * right_along), keepdims=True)

    def unit(index, k):
        return (index == k).astype(jnp.float32)

    q_d, q_a = unit(i, 0), unit(j, 0)
    w_d, w_a = unit(i, S + 1), unit(j, S + 1)
    c_d = jnp.zeros(shape, jnp.float32)
    rho = quadratic(w_d, w_a)
    for _ in range(S):
        m_d, m_a = down(q_d), along(q_a)
        alpha = rho / quadratic(q_d, m_a)
        c_d = c_d + alpha * q_d
        w_d, w_a = w_d - alpha * m_d, w_a - alpha * m_a
        rho_new = quadratic(w_d, w_a)
        beta = rho_new / rho
        q_d, q_a = w_d + beta * q_d, w_a + beta * q_a
        rho = rho_new
    return c_d, w_d, q_d


def combine(k, coefs, chain_d, chain_r, out):
    per, keep = out.shape[1], out.shape[3]
    core, _ = here()
    first = per * piece_of(k)
    tile = 16

    def body(step, _):
        plane, at = step // (keep // tile), step % (keep // tile)
        row = pl.multiple_of(at * tile, tile)
        source = pl.ds(pl.multiple_of(PAD + HALO + row, 8), tile)
        where = HALO + jnp.where(core == 0, first + plane, PLANES - 1 - first - plane)
        sums = [[None] * 3, [None] * 3]
        for column in range(COLS):
            chain, power, steps = (chain_d, column, S) if column <= S else (chain_r, column - S - 1, S - 1)
            low = chain_plan(steps)[0][power]
            factors = [coefs[which, column : column + 1, :] for which in range(3)]
            for h in range(2):
                v = chain[power][where - low, h, source]
                for which in range(3):
                    term = v * factors[which]
                    sums[h][which] = term if column == 0 else sums[h][which] + term
        for h in range(2):
            for which in range(3):
                out[which, plane, h, pl.ds(row, tile)] = sums[h][which]
        return 0

    lax.fori_loop(0, per * (keep // tile), body, 0)


def first_combine_kernel(k, sums, *refs):
    chain_d, chain_r, out, coefs = refs[: S + 1], refs[S + 1 : COLS], refs[COLS], refs[COLS + 1]
    total = jnp.sum(sums[...], axis=0, keepdims=True)
    for which, value in enumerate(coefficients(total)):
        coefs[which] = value
    combine(k, coefs, chain_d, chain_r, out)


def combine_kernel(k, coefs, *refs):
    combine(k, coefs, refs[: S + 1], refs[S + 1 : COLS], refs[COLS])


def finish_kernel(solution, *refs):
    pieces, outs, hold, sem = refs[:PIECES], refs[PIECES : PIECES + 3], refs[PIECES + 3], refs[PIECES + 4]
    _, per, halves, keep, _ = pieces[0].shape
    copies = []
    for which in (1, 2, 0):
        for k in range(PIECES):
            rows = pl.ds(pl.multiple_of(piece_of(PIECES - k) * keep, keep), keep)
            for h in range(halves):
                for plane in range(per):
                    value = pieces[k][which, plane, h]
                    where = (plane, rows, pl.ds(h * HALF, HALF))
                    if which == 0:
                        value = value + solution[where]
                    hold[(which, *where)] = value
        copies.append(pltpu.make_async_copy(hold.at[which], outs[which], sem.at[which]))
        copies[-1].start()
    for copy in copies:
        copy.wait()


def on_device(solution, residual, direction):
    groups = lax.axis_size("x")
    outer = lax.axis_size("zz")
    per, height, lanes = direction.shape
    keep = height // groups
    rows = keep + 2 * HALO
    f32 = jnp.float32

    blocks = 2 * outer
    near = [(b, b - 1) for b in range(0, blocks, 2) if b > 0] + [(b, b + 1) for b in range(1, blocks, 2) if b + 1 < blocks]

    def params(mib=4):
        return pltpu.CompilerParams(vmem_limit_bytes=mib * 2**20)

    def cost(us):
        return pl.CostEstimate(flops=us * 10**7, bytes_accessed=0, transcendentals=0)

    def ahead(value, k):
        return lax.ppermute(value, "x", [(i, (i + k) % groups) for i in range(groups)])

    def spread(field, after):
        pieces = pl.pallas_call(
            pack_kernel,
            out_shape=(jax.ShapeDtypeStruct((per, 2, rows, HALF), f32),) * groups,
            in_specs=[VMEM] + [HBM] * len(after),
            out_specs=(VMEM,) * groups,
            compiler_params=params(1),
            name="pack",
        )(field, *after)
        got = [pieces[0]] + [ahead(pieces[k], k) for k in range(1, groups)]
        own = pl.pallas_call(
            join_kernel,
            out_shape=jax.ShapeDtypeStruct((groups, per, 2, rows, HALF), f32),
            in_specs=[VMEM] * groups,
            out_specs=VMEM,
            compiler_params=params(1),
            name="join",
        )(*got)
        across = lax.ppermute(own, ("zz", "c"), near)
        side = lax.ppermute(own, "c", [(0, 1), (1, 0)])
        return own, side, across

    def chain_shapes(steps):
        return tuple(
            jax.ShapeDtypeStruct((end - low, 2, rows + 2 * PAD, HALF), f32) for low, end in zip(*chain_plan(steps))
        )

    sideways = pltpu.VMEM((GROUP, 2, rows, HALF), f32)

    def near_chain(steps, own, side):
        return pl.pallas_call(
            functools.partial(near_kernel, steps),
            out_shape=chain_shapes(steps),
            in_specs=[VMEM] * 2,
            out_specs=(VMEM,) * (steps + 1),
            scratch_shapes=[sideways],
            compiler_params=params(),
            cost_estimate=cost(4),
            name="near_chain",
        )(own, side)

    own_d, side_d, across_d = spread(direction, ())
    own_r, side_r, across_r = spread(residual, (own_d,))
    chain_d = near_chain(S, own_d, side_d)
    *chain_d, parts = pl.pallas_call(
        far_direction_kernel,
        out_shape=(*chain_shapes(S), jax.ShapeDtypeStruct((128, 128), f32)),
        in_specs=[VMEM] * (S + 2),
        out_specs=(VMEM,) * (S + 2),
        scratch_shapes=[sideways, pltpu.VMEM((2 * S + 1, 8, HALF), f32)],
        input_output_aliases={1 + k: k for k in range(S + 1)},
        compiler_params=params(),
        cost_estimate=cost(4),
        name="far_direction",
    )(across_d, *chain_d)
    chain_r = near_chain(S - 1, own_r, side_r)
    *chain_r, sums = pl.pallas_call(
        far_residual_kernel,
        out_shape=(*chain_shapes(S - 1), jax.ShapeDtypeStruct((1, 128), f32)),
        in_specs=[VMEM] * (2 * S + 3),
        out_specs=(VMEM,) * (S + 1),
        scratch_shapes=[sideways, pltpu.VMEM((4 * S - 1, 8, HALF), f32), pltpu.VMEM((128, 128), f32)],
        input_output_aliases={S + 3 + k: k for k in range(S)},
        compiler_params=params(),
        cost_estimate=cost(4),
        name="far_residual",
    )(across_r, *chain_d, parts, *chain_r)

    devices = groups * blocks
    everyone = lax.all_to_all(jnp.broadcast_to(sums[None], (devices, 1, 128)), ALL, 0, 0, tiled=True)

    mixed_shape = jax.ShapeDtypeStruct((3, per, 2, keep, HALF), f32)
    mixed = {}
    first, *others = (2, 1, 3, 0)
    mixed[first], coefs = pl.pallas_call(
        functools.partial(first_combine_kernel, first),
        out_shape=(mixed_shape, jax.ShapeDtypeStruct((3, 24, 128), f32)),
        in_specs=[VMEM] * (COLS + 1),
        out_specs=(VMEM, VMEM),
        compiler_params=params(),
        cost_estimate=cost(4),
        name="combine",
    )(everyone.reshape(devices, 128), *chain_d, *chain_r)
    for k in others:
        mixed[k] = pl.pallas_call(
            functools.partial(combine_kernel, k),
            out_shape=mixed_shape,
            in_specs=[VMEM] * (COLS + 1),
            out_specs=VMEM,
            compiler_params=params(),
            cost_estimate=cost(1),
            name="combine",
        )(coefs, *chain_d, *chain_r)
    back = [mixed[k] if k == 0 else ahead(mixed[k], k) for k in range(groups)]

    whole = jax.ShapeDtypeStruct((per, height, lanes), f32)
    return pl.pallas_call(
        finish_kernel,
        out_shape=(whole,) * 3,
        in_specs=[VMEM] * (groups + 1),
        out_specs=(HBM,) * 3,
        scratch_shapes=[pltpu.VMEM((3, per, height, lanes), f32), pltpu.SemaphoreType.DMA((3,))],
        compiler_params=params(8),
        name="finish",
    )(solution, *back)


def solution(mesh):
    blocks, groups = mesh.devices.shape
    split = Mesh(mesh.devices.reshape(blocks // 2, 2, groups), ALL)
    spec = P(ALL, None, None)
    return jax.shard_map(
        on_device, mesh=split, in_specs=(spec, spec, spec), out_specs=(spec, spec, spec), check_vma=False
    )
```

```python
import functools

import jax
import jax.numpy as jnp
from jax import lax
from jax.experimental import pallas as pl
from jax.experimental.pallas import tpu as pltpu
from jax.sharding import Mesh, PartitionSpec as P


S = 8
PIECES = 4
COLS = 2 * S + 1
PLANES = 8
HALO = 8
TALL = PLANES + 2 * HALO
PAD = 8
HALF = 128
GROUP = 4
FIRST = -1.0 / 6.0
NEXT = -1.0 / 3.0
ALL = ("zz", "c", "x")
VMEM = pl.BlockSpec(memory_space=pltpu.VMEM)
HBM = pl.BlockSpec(memory_space=pltpu.HBM)

DD, RR, DR = 0, 2 * S + 1, 4 * S
SUMS = 6 * S


def here():
    return lax.axis_index("c"), lax.axis_index("x")


def piece_of(k):
    return (lax.axis_index("x") + k) % PIECES


def chain_plan(steps):
    lows = [0] + [HALO - steps + k for k in range(1, steps + 1)]
    ends = [TALL] + [HALO + PLANES + steps - k for k in range(1, steps + 1)]
    return lows, ends


def parting(back):
    i = lax.broadcasted_iota(jnp.int32, (2 * HALF, 2 * HALF), 0 if back else 1)
    j = lax.broadcasted_iota(jnp.int32, (2 * HALF, 2 * HALF), 1 if back else 0)
    return (j == jnp.where(i < HALF, 2 * i, 2 * (i - HALF) + 1)).astype(jnp.float32)


def move_columns(value, matrix):
    return jnp.dot(value, matrix, precision=lax.Precision.HIGHEST, preferred_element_type=jnp.float32)


def pack_kernel(source, *refs):
    outs, hold = refs[:PIECES], refs[PIECES]
    per, halves, rows, _ = outs[0].shape
    keep, height = rows - 2 * HALO, source.shape[1]
    matrix = parting(False)
    for plane in range(per):
        parted = move_columns(source[plane], matrix)
        for h in range(halves):
            hold[plane, h] = parted[:, h * HALF : (h + 1) * HALF]
    for k in range(PIECES):
        g = piece_of(k)
        row = pl.multiple_of(g * keep, keep)
        below = pl.multiple_of(jnp.maximum(row - HALO, 0), HALO)
        above = pl.multiple_of(jnp.minimum(row + keep, height - HALO), HALO)
        has_below, has_above = (g != 0).astype(jnp.float32), (g != PIECES - 1).astype(jnp.float32)
        for plane in range(per):
            for h in range(halves):
                outs[k][plane, h, :HALO] = hold[plane, h, pl.ds(below, HALO)] * has_below
                outs[k][plane, h, pl.ds(HALO, keep)] = hold[plane, h, pl.ds(row, keep)]
                outs[k][plane, h, rows - HALO :] = hold[plane, h, pl.ds(above, HALO)] * has_above


def join_kernel(*refs):
    out = refs[PIECES]
    core, _ = here()
    per = refs[0].shape[0]
    for k in range(PIECES):
        plane = per * piece_of(PIECES - k)
        for p in range(per):
            out[jnp.where(core == 0, plane + p, PLANES - 1 - plane - p)] = refs[k][p]


def load_planes(chain, source, places):
    rows = pl.ds(PAD, source.shape[2])
    for i, place in enumerate(places):
        for h in range(2):
            chain[0][place, h, rows] = source[i, h]


def run_groups(groups, chain, sideways, rows, steps):
    lows, _ = chain_plan(steps)
    data = pl.ds(PAD, rows)
    core, x = here()
    zz = lax.axis_index("zz")
    last = lax.axis_size("zz") - 1
    alone = jnp.logical_or(jnp.logical_and(zz == 0, core == 0), jnp.logical_and(zz == last, core == 1))
    low_x = (x != 0).astype(jnp.float32)
    high_x = (x != PIECES - 1).astype(jnp.float32)
    across_valid = 1.0 - alone.astype(jnp.float32)
    lane = lax.broadcasted_iota(jnp.int32, (rows, HALF), 1)
    at_low, at_high = lane == 0, lane == HALF - 1

    def neighbours_y(power, plane):
        source = chain[power - 1]
        index = plane - lows[power - 1]
        a, b = source[index, 0, data], source[index, 1, data]
        first = b + jnp.where(at_low, 0.0, pltpu.roll(b, 1, 1))
        second = a + jnp.where(at_high, 0.0, pltpu.roll(a, HALF - 1, 1))
        return first, second

    def value(power, plane, slot, across):
        now, new = chain[power - 1], chain[power]
        index = plane - lows[power - 1]
        scale = FIRST if power == 1 else NEXT
        if across:
            scale = scale * across_valid
        for h in range(2):
            total = now[index - 1, h, data] + now[index + 1, h, data]
            total = total + (now[index, h, pl.ds(PAD - 1, rows)] + now[index, h, pl.ds(PAD + 1, rows)])
            total = total + sideways[slot, h]
            parts = []
            for a, b, weight in ((0, HALO, low_x), (HALO, rows - HALO, None), (rows - HALO, rows, high_x)):
                parts.append(total[a:b] * (scale if weight is None else scale * weight))
            result = jnp.concatenate(parts, axis=0)
            if power > 1:
                result = result - chain[power - 2][plane - lows[power - 2], h, data]
            new[plane - lows[power], h, data] = result

    def step(group, then):
        power, plane, count = group
        made = [(power, plane + u) for u in range(count)] if isinstance(plane, int) else []
        ahead, late = [], []
        if then:
            for u in range(then[2]):
                if (then[0] - 1, then[1] + u) in made:
                    late.append(u)
                else:
                    ahead.append((u, neighbours_y(then[0], then[1] + u)))
        for u in range(count):
            value(power, plane + u, u, isinstance(plane, int) and plane + u < HALO)
        ahead += [(u, neighbours_y(then[0], then[1] + u)) for u in late]
        for u, pair in ahead:
            sideways[u, 0], sideways[u, 1] = pair

    first = groups[0]
    for u in range(first[2]):
        sideways[u, 0], sideways[u, 1] = neighbours_y(first[0], first[1] + u)
    at = 0
    while at < len(groups):
        power, plane, count = groups[at]
        run = 0
        while at + run + 1 < len(groups) and groups[at + run + 1] == (power, plane + GROUP * (run + 1), count) and count == GROUP:
            run += 1
        if run >= 2:

            def body(g, _, power=power, plane=plane):
                now = plane + GROUP * g
                step((power, now, GROUP), (power, now + GROUP, GROUP))
                return 0

            lax.fori_loop(0, run, body, 0)
            at += run
        step(groups[at], groups[at + 1] if at + 1 < len(groups) else None)
        at += 1


def near_groups(steps):
    _, ends = chain_plan(steps)
    groups = []
    for power in range(1, steps + 1):
        low, end = HALO + power, ends[power]
        left = end - low
        while left > 0:
            count = min(GROUP, left)
            if left in (5, 6):
                count = 3
            groups.append((power, low, count))
            low, left = low + count, left - count
    return groups


def far_groups(steps):
    lows, _ = chain_plan(steps)
    groups = []
    for power in range(1, steps + 1):
        middle = HALO + power - GROUP
        groups.append((power, middle, GROUP))
        groups.append((power, lows[power], middle - lows[power]))
    return groups


def near_kernel(steps, own, side, *refs):
    chain, sideways = refs[: steps + 1], refs[steps + 1]
    load_planes(chain, own, range(HALO, HALO + PLANES))
    load_planes(chain, side, range(TALL - 1, HALO + PLANES - 1, -1))
    run_groups(near_groups(steps), chain, sideways, own.shape[2], steps)


def add_products(acc, chain, steps, other, keep):
    rows = pl.ds(PAD + HALO, keep)
    acc[...] = jnp.zeros_like(acc)

    def total(a, b):
        return jnp.sum((a * b).reshape(keep // 8, 8, HALF), axis=0)

    def body(step, _):
        plane, h = step // 2, step % 2

        def of(chain, steps, k):
            return chain[k][HALO + plane - chain_plan(steps)[0][k], h, rows]

        before, beside = None, None
        if other:
            beside = of(other, S, 0)
        for k in range(steps + 1):
            now = of(chain, steps, k)
            acc[2 * k] += total(now, now)
            if k:
                acc[2 * k - 1] += total(before, now)
            if other:
                following = of(other, S, k + 1)
                acc[2 * steps + 1 + 2 * k] += total(beside, now)
                acc[2 * steps + 2 + 2 * k] += total(following, now)
                beside = following
            before = now
        return 0

    lax.fori_loop(0, 2 * PLANES, body, 0)


def put_products(acc, parts, place):
    for k in range(acc.shape[0]):
        parts[pl.ds(place + k, 1), :] = jnp.sum(acc[k], axis=0, keepdims=True)


def far_direction_kernel(across, *refs):
    chain, parts, sideways, acc = refs[S + 1 : 2 * S + 2], refs[2 * S + 2], refs[2 * S + 3], refs[2 * S + 4]
    rows = across.shape[2]
    load_planes(chain, across, range(HALO - 1, HALO - 1 - across.shape[0], -1))
    run_groups(far_groups(S), chain, sideways, rows, S)
    add_products(acc, chain, S, None, rows - 2 * HALO)
    parts[...] = jnp.zeros_like(parts)
    put_products(acc, parts, DD)


def far_residual_kernel(across, *refs):
    other, parts_d, refs = refs[: S + 1], refs[S + 1], refs[S + 2 :]
    chain, sums, sideways, acc, parts = refs[S : 2 * S], refs[2 * S], refs[2 * S + 1], refs[2 * S + 2], refs[2 * S + 3]
    rows = across.shape[2]
    load_planes(chain, across, range(HALO - 1, HALO - 1 - across.shape[0], -1))
    run_groups(far_groups(S - 1), chain, sideways, rows, S - 1)
    add_products(acc, chain, S - 1, other, rows - 2 * HALO)
    parts[...] = parts_d[...]
    put_products(acc, parts, RR)
    sums[...] = jnp.sum(parts[...].T, axis=0, keepdims=True)


def coefficients(sums):
    tall = 24
    shape = (tall, 128)
    i = lax.broadcasted_iota(jnp.int32, shape, 0)
    j = lax.broadcasted_iota(jnp.int32, shape, 1)
    row_r, col_r = i > S, j > S
    a = jnp.where(row_r, i - (S + 1), i)
    b = jnp.where(col_r, j - (S + 1), j)
    valid = jnp.logical_and(i < COLS, j < COLS)
    base = jnp.where(row_r, jnp.where(col_r, RR, DR), jnp.where(col_r, DR, DD))
    at_plus = jnp.where(valid, base + a + b, -1)
    at_minus = jnp.where(valid, base + jnp.abs(a - b), -1)
    at_base = jnp.where(valid, base + ((a + b) & 1), -1)
    gram = jnp.zeros(shape, jnp.float32)
    for place in range(SUMS):
        weight = (
            (at_plus == place).astype(jnp.float32)
            + (at_minus == place).astype(jnp.float32)
            - (at_base == place).astype(jnp.float32)
        )
        gram = gram + weight * sums[:, place : place + 1]

    def change(index, axis):
        second = index > S
        k = jnp.where(second, index - (S + 1), index)
        count = jnp.where(second, S, S + 1)
        valid = index < COLS
        middle = jnp.where(jnp.logical_and(valid, k < count - 1), 6.0, 0.0)
        below = jnp.where(jnp.logical_and(valid, k >= 1), jnp.where(k == 1, 6.0, 3.0), 0.0)
        above = jnp.where(jnp.logical_and(valid, k + 1 < count - 1), 3.0, 0.0)
        size = shape[axis]

        def apply(v):
            return middle * v + below * pltpu.roll(v, 1, axis) + above * pltpu.roll(v, size - 1, axis)

        return apply

    down, along = change(i, 0), change(j, 1)

    def quadratic(left_down, right_along):
        return jnp.sum(left_down * (gram * right_along), keepdims=True)

    def unit(index, k):
        return (index == k).astype(jnp.float32)

    q_d, q_a = unit(i, 0), unit(j, 0)
    w_d, w_a = unit(i, S + 1), unit(j, S + 1)
    c_d = jnp.zeros(shape, jnp.float32)
    rho = quadratic(w_d, w_a)
    for _ in range(S):
        m_d, m_a = down(q_d), along(q_a)
        alpha = rho / quadratic(q_d, m_a)
        c_d = c_d + alpha * q_d
        w_d, w_a = w_d - alpha * m_d, w_a - alpha * m_a
        rho_new = quadratic(w_d, w_a)
        beta = rho_new / rho
        q_d, q_a = w_d + beta * q_d, w_a + beta * q_a
        rho = rho_new
    return c_d, w_d, q_d


def combine(k, coefs, chain_d, chain_r, out, hold):
    per, keep = out.shape[1], out.shape[2]
    core, _ = here()
    first = per * piece_of(k)
    tile = 16

    def body(step, _):
        plane, at = step // (keep // tile), step % (keep // tile)
        row = pl.multiple_of(at * tile, tile)
        source = pl.ds(pl.multiple_of(PAD + HALO + row, 8), tile)
        where = HALO + jnp.where(core == 0, first + plane, PLANES - 1 - first - plane)
        sums = [[None] * 3, [None] * 3]
        for column in range(COLS):
            chain, power, steps = (chain_d, column, S) if column <= S else (chain_r, column - S - 1, S - 1)
            low = chain_plan(steps)[0][power]
            factors = [coefs[which, column : column + 1, :] for which in range(3)]
            for h in range(2):
                v = chain[power][where - low, h, source]
                for which in range(3):
                    term = v * factors[which]
                    sums[h][which] = term if column == 0 else sums[h][which] + term
        for h in range(2):
            for which in range(3):
                to = pl.multiple_of((which * per + plane) * keep + row, tile)
                hold[pl.ds(to, tile), h * HALF : (h + 1) * HALF] = sums[h][which]
        return 0

    lax.fori_loop(0, per * (keep // tile), body, 0)
    out[...] = move_columns(hold[...], parting(True)).reshape(out.shape)


def first_combine_kernel(k, sums, *refs):
    chain_d, chain_r, out, coefs, hold = refs[: S + 1], refs[S + 1 : COLS], *refs[COLS:]
    total = jnp.sum(sums[...], axis=0, keepdims=True)
    for which, value in enumerate(coefficients(total)):
        coefs[which] = value
    combine(k, coefs, chain_d, chain_r, out, hold)


def combine_kernel(k, coefs, *refs):
    combine(k, coefs, refs[: S + 1], refs[S + 1 : COLS], *refs[COLS:])


def finish_kernel(solution, *refs):
    pieces, outs, hold, sem = refs[:PIECES], refs[PIECES : PIECES + 3], refs[PIECES + 3], refs[PIECES + 4]
    _, per, keep, _ = pieces[0].shape
    copies = []
    for which in (1, 2, 0):
        for k in range(PIECES):
            rows = pl.ds(pl.multiple_of(piece_of(PIECES - k) * keep, keep), keep)
            for plane in range(per):
                value = pieces[k][which, plane]
                if which == 0:
                    value = value + solution[plane, rows]
                hold[which, plane, rows] = value
        copies.append(pltpu.make_async_copy(hold.at[which], outs[which], sem.at[which]))
        copies[-1].start()
    for copy in copies:
        copy.wait()


def on_device(solution, residual, direction):
    groups = lax.axis_size("x")
    outer = lax.axis_size("zz")
    per, height, lanes = direction.shape
    keep = height // groups
    rows = keep + 2 * HALO
    f32 = jnp.float32

    blocks = 2 * outer
    near = [(b, b - 1) for b in range(0, blocks, 2) if b > 0] + [(b, b + 1) for b in range(1, blocks, 2) if b + 1 < blocks]

    def params(mib=4):
        return pltpu.CompilerParams(vmem_limit_bytes=mib * 2**20)

    def cost(us):
        return pl.CostEstimate(flops=us * 10**7, bytes_accessed=0, transcendentals=0)

    def ahead(value, k):
        return lax.ppermute(value, "x", [(i, (i + k) % groups) for i in range(groups)])

    def spread(field, reach):
        pieces = pl.pallas_call(
            pack_kernel,
            out_shape=(jax.ShapeDtypeStruct((per, 2, rows, HALF), f32),) * groups,
            in_specs=[VMEM],
            out_specs=(VMEM,) * groups,
            scratch_shapes=[pltpu.VMEM((per, 2, height, HALF), f32)],
            compiler_params=params(),
            name="pack",
        )(field)
        got = [pieces[0]]
        for k in range(1, groups):
            got.append(ahead(pieces[k], k))
        own = pl.pallas_call(
            join_kernel,
            out_shape=jax.ShapeDtypeStruct((PLANES, 2, rows, HALF), f32),
            in_specs=[VMEM] * groups,
            out_specs=VMEM,
            compiler_params=params(1),
            name="join",
        )(*got)
        side = lax.ppermute(own, "c", [(0, 1), (1, 0)])
        across = lax.ppermute(own[:reach], ("zz", "c"), near)
        return own, side, across

    def chain_shapes(steps):
        return tuple(
            jax.ShapeDtypeStruct((end - low, 2, rows + 2 * PAD, HALF), f32) for low, end in zip(*chain_plan(steps))
        )

    sideways = pltpu.VMEM((GROUP, 2, rows, HALF), f32)

    def near_chain(steps, own, side):
        return pl.pallas_call(
            functools.partial(near_kernel, steps),
            out_shape=chain_shapes(steps),
            in_specs=[VMEM] * 2,
            out_specs=(VMEM,) * (steps + 1),
            scratch_shapes=[sideways],
            compiler_params=params(),
            cost_estimate=cost(4),
            name="near_chain",
        )(own, side)

    own_d, side_d, across_d = spread(direction, S)
    own_r, side_r, across_r = spread(residual, S - 1)
    chain_d = near_chain(S, own_d, side_d)
    *chain_d, parts = pl.pallas_call(
        far_direction_kernel,
        out_shape=(*chain_shapes(S), jax.ShapeDtypeStruct((128, 128), f32)),
        in_specs=[VMEM] * (S + 2),
        out_specs=(VMEM,) * (S + 2),
        scratch_shapes=[sideways, pltpu.VMEM((2 * S + 1, 8, HALF), f32)],
        input_output_aliases={1 + k: k for k in range(S + 1)},
        compiler_params=params(),
        cost_estimate=cost(4),
        name="far_direction",
    )(across_d, *chain_d)
    chain_r = near_chain(S - 1, own_r, side_r)
    *chain_r, sums = pl.pallas_call(
        far_residual_kernel,
        out_shape=(*chain_shapes(S - 1), jax.ShapeDtypeStruct((1, 128), f32)),
        in_specs=[VMEM] * (2 * S + 3),
        out_specs=(VMEM,) * (S + 1),
        scratch_shapes=[sideways, pltpu.VMEM((4 * S - 1, 8, HALF), f32), pltpu.VMEM((128, 128), f32)],
        input_output_aliases={S + 3 + k: k for k in range(S)},
        compiler_params=params(),
        cost_estimate=cost(4),
        name="far_residual",
    )(across_r, *chain_d, parts, *chain_r)

    devices = groups * blocks
    everyone = lax.all_to_all(jnp.broadcast_to(sums[None], (devices, 1, 128)), ALL, 0, 0, tiled=True)

    mixed_shape = jax.ShapeDtypeStruct((3, per, keep, lanes), f32)
    hold = pltpu.VMEM((3 * per * keep, lanes), f32)
    mixed = {}
    first, *others = (2, 1, 3, 0)
    mixed[first], coefs = pl.pallas_call(
        functools.partial(first_combine_kernel, first),
        out_shape=(mixed_shape, jax.ShapeDtypeStruct((3, 24, 128), f32)),
        in_specs=[VMEM] * (COLS + 1),
        out_specs=(VMEM, VMEM),
        scratch_shapes=[hold],
        compiler_params=params(),
        cost_estimate=cost(4),
        name="combine",
    )(everyone.reshape(devices, 128), *chain_d, *chain_r)
    for k in others:
        mixed[k] = pl.pallas_call(
            functools.partial(combine_kernel, k),
            out_shape=mixed_shape,
            in_specs=[VMEM] * (COLS + 1),
            out_specs=VMEM,
            scratch_shapes=[hold],
            compiler_params=params(),
            cost_estimate=cost(1),
            name="combine",
        )(coefs, *chain_d, *chain_r)
    back = [mixed[0]]
    for k in range(1, groups):
        back.append(ahead(mixed[k], k))

    whole = jax.ShapeDtypeStruct((per, height, lanes), f32)
    return pl.pallas_call(
        finish_kernel,
        out_shape=(whole,) * 3,
        in_specs=[VMEM] * (groups + 1),
        out_specs=(HBM,) * 3,
        scratch_shapes=[pltpu.VMEM((3, per, height, lanes), f32), pltpu.SemaphoreType.DMA((3,))],
        compiler_params=params(8),
        name="finish",
    )(solution, *back)


def solution(mesh):
    blocks, groups = mesh.devices.shape
    split = Mesh(mesh.devices.reshape(blocks // 2, 2, groups), ALL)
    spec = P(ALL, None, None)

    return jax.shard_map(
        on_device, mesh=split, in_specs=(spec, spec, spec), out_specs=(spec, spec, spec), check_vma=False
    )
```

```python
import functools

import jax
import jax.numpy as jnp
from jax import lax
from jax.experimental import pallas as pl
from jax.experimental.pallas import tpu as pltpu
from jax.sharding import Mesh, PartitionSpec as P


S = 8
PIECES = 4
COLS = 2 * S + 1
PLANES = 8
HALO = 8
TALL = PLANES + 2 * HALO
PAD = 8
HALF = 128
GROUP = 4
FIRST = -1.0 / 6.0
NEXT = -1.0 / 3.0
ALL = ("zz", "c", "x")
VMEM = pl.BlockSpec(memory_space=pltpu.VMEM)
HBM = pl.BlockSpec(memory_space=pltpu.HBM)

DD, RR, DR = 0, 2 * S + 1, 4 * S
SUMS = 6 * S


def here():
    return lax.axis_index("c"), lax.axis_index("x")


def piece_of(k):
    return (lax.axis_index("x") + k) % PIECES


def chain_plan(steps):
    lows = [0] + [HALO - steps + k for k in range(1, steps + 1)]
    ends = [TALL] + [HALO + PLANES + steps - k for k in range(1, steps + 1)]
    return lows, ends


def parting(back):
    i = lax.broadcasted_iota(jnp.int32, (2 * HALF, 2 * HALF), 0 if back else 1)
    j = lax.broadcasted_iota(jnp.int32, (2 * HALF, 2 * HALF), 1 if back else 0)
    return (j == jnp.where(i < HALF, 2 * i, 2 * (i - HALF) + 1)).astype(jnp.bfloat16)


def move_columns(value, matrix):
    total = None
    for _ in range(3):
        part = value.astype(jnp.bfloat16)
        moved = jnp.dot(part, matrix, preferred_element_type=jnp.float32)
        total = moved if total is None else total + moved
        value = value - part.astype(jnp.float32)
    return total


def part_columns(source, out):
    matrix = parting(False)
    for plane in range(source.shape[0]):
        parted = move_columns(source[plane], matrix)
        for h in range(2):
            out[plane, h] = parted[:, h * HALF : (h + 1) * HALF]


def pack_kernel(source, *refs):
    part_columns(source, refs[PIECES])
    cut_kernel(refs[PIECES], *refs[:PIECES])


def cut_kernel(planes, *outs):
    per, halves, rows, _ = outs[0].shape
    keep, height = rows - 2 * HALO, planes.shape[2]
    for k in range(PIECES):
        g = piece_of(k)
        row = pl.multiple_of(g * keep, keep)
        below = pl.multiple_of(jnp.maximum(row - HALO, 0), HALO)
        above = pl.multiple_of(jnp.minimum(row + keep, height - HALO), HALO)
        has_below, has_above = (g != 0).astype(jnp.float32), (g != PIECES - 1).astype(jnp.float32)
        for plane in range(per):
            for h in range(halves):
                outs[k][plane, h, :HALO] = planes[plane, h, pl.ds(below, HALO)] * has_below
                outs[k][plane, h, pl.ds(HALO, keep)] = planes[plane, h, pl.ds(row, keep)]
                outs[k][plane, h, rows - HALO :] = planes[plane, h, pl.ds(above, HALO)] * has_above


def join_kernel(mirrored, *refs):
    out = refs[PIECES]
    core, _ = here()
    core = 1 - core if mirrored else core
    per = refs[0].shape[0]
    for k in range(PIECES):
        plane = per * piece_of(PIECES - k)
        for p in range(per):
            out[jnp.where(core == 0, plane + p, PLANES - 1 - plane - p)] = refs[k][p]


def load_planes(chain, source, places):
    rows = pl.ds(PAD, source.shape[2])
    for i, place in enumerate(places):
        for h in range(2):
            chain[0][place, h, rows] = source[i, h]


def run_groups(groups, chain, sideways, rows, steps):
    lows, _ = chain_plan(steps)
    data = pl.ds(PAD, rows)
    core, x = here()
    zz = lax.axis_index("zz")
    last = lax.axis_size("zz") - 1
    alone = jnp.logical_or(jnp.logical_and(zz == 0, core == 0), jnp.logical_and(zz == last, core == 1))
    low_x = (x != 0).astype(jnp.float32)
    high_x = (x != PIECES - 1).astype(jnp.float32)
    across_valid = 1.0 - alone.astype(jnp.float32)
    lane = lax.broadcasted_iota(jnp.int32, (rows, HALF), 1)
    at_low, at_high = lane == 0, lane == HALF - 1

    def neighbours_y(power, plane):
        source = chain[power - 1]
        index = plane - lows[power - 1]
        a, b = source[index, 0, data], source[index, 1, data]
        first = b + jnp.where(at_low, 0.0, pltpu.roll(b, 1, 1))
        second = a + jnp.where(at_high, 0.0, pltpu.roll(a, HALF - 1, 1))
        return first, second

    def value(power, plane, slot, across):
        now, new = chain[power - 1], chain[power]
        index = plane - lows[power - 1]
        scale = FIRST if power == 1 else NEXT
        if across:
            scale = scale * across_valid
        for h in range(2):
            total = now[index - 1, h, data] + now[index + 1, h, data]
            total = total + (now[index, h, pl.ds(PAD - 1, rows)] + now[index, h, pl.ds(PAD + 1, rows)])
            total = total + sideways[slot, h]
            parts = []
            for a, b, weight in ((0, HALO, low_x), (HALO, rows - HALO, None), (rows - HALO, rows, high_x)):
                parts.append(total[a:b] * (scale if weight is None else scale * weight))
            result = jnp.concatenate(parts, axis=0)
            if power > 1:
                result = result - chain[power - 2][plane - lows[power - 2], h, data]
            new[plane - lows[power], h, data] = result

    def step(group, then):
        power, plane, count = group
        made = [(power, plane + u) for u in range(count)] if isinstance(plane, int) else []
        ahead, late = [], []
        if then:
            for u in range(then[2]):
                if (then[0] - 1, then[1] + u) in made:
                    late.append(u)
                else:
                    ahead.append((u, neighbours_y(then[0], then[1] + u)))
        for u in range(count):
            value(power, plane + u, u, isinstance(plane, int) and plane + u < HALO)
        ahead += [(u, neighbours_y(then[0], then[1] + u)) for u in late]
        for u, pair in ahead:
            sideways[u, 0], sideways[u, 1] = pair

    first = groups[0]
    for u in range(first[2]):
        sideways[u, 0], sideways[u, 1] = neighbours_y(first[0], first[1] + u)
    at = 0
    while at < len(groups):
        power, plane, count = groups[at]
        run = 0
        while at + run + 1 < len(groups) and groups[at + run + 1] == (power, plane + GROUP * (run + 1), count) and count == GROUP:
            run += 1
        if run >= 2:

            def body(g, _, power=power, plane=plane):
                now = plane + GROUP * g
                step((power, now, GROUP), (power, now + GROUP, GROUP))
                return 0

            lax.fori_loop(0, run, body, 0)
            at += run
        step(groups[at], groups[at + 1] if at + 1 < len(groups) else None)
        at += 1


def near_groups(steps):
    _, ends = chain_plan(steps)
    groups = []
    for power in range(1, steps + 1):
        low, end = HALO + power, ends[power]
        left = end - low
        while left > 0:
            count = min(GROUP, left)
            if left in (5, 6):
                count = 3
            groups.append((power, low, count))
            low, left = low + count, left - count
    return groups


def far_groups(steps):
    lows, _ = chain_plan(steps)
    groups = []
    for power in range(1, steps + 1):
        middle = HALO + power - GROUP
        groups.append((power, middle, GROUP))
        groups.append((power, lows[power], middle - lows[power]))
    return groups


def near_kernel(steps, own, side, *refs):
    chain, sideways = refs[: steps + 1], refs[steps + 1]
    load_planes(chain, own, range(HALO, HALO + PLANES))
    load_planes(chain, side, range(TALL - 1, HALO + PLANES - 1, -1))
    run_groups(near_groups(steps), chain, sideways, own.shape[2], steps)


def add_products(acc, chain, steps, other, keep):
    rows = pl.ds(PAD + HALO, keep)
    acc[...] = jnp.zeros_like(acc)

    def total(a, b):
        return jnp.sum((a * b).reshape(keep // 8, 8, HALF), axis=0)

    def body(step, _):
        plane, h = step // 2, step % 2

        def of(chain, steps, k):
            return chain[k][HALO + plane - chain_plan(steps)[0][k], h, rows]

        before, beside = None, None
        if other:
            beside = of(other, S, 0)
        for k in range(steps + 1):
            now = of(chain, steps, k)
            acc[2 * k] += total(now, now)
            if k:
                acc[2 * k - 1] += total(before, now)
            if other:
                following = of(other, S, k + 1)
                acc[2 * steps + 1 + 2 * k] += total(beside, now)
                acc[2 * steps + 2 + 2 * k] += total(following, now)
                beside = following
            before = now
        return 0

    lax.fori_loop(0, 2 * PLANES, body, 0)


def put_products(acc, parts, place):
    for k in range(acc.shape[0]):
        parts[pl.ds(place + k, 1), :] = jnp.sum(acc[k], axis=0, keepdims=True)


def far_direction_kernel(across, *refs):
    chain, parts, sideways, acc = refs[S + 1 : 2 * S + 2], refs[2 * S + 2], refs[2 * S + 3], refs[2 * S + 4]
    rows = across.shape[2]
    load_planes(chain, across, range(HALO - 1, HALO - 1 - across.shape[0], -1))
    run_groups(far_groups(S), chain, sideways, rows, S)
    add_products(acc, chain, S, None, rows - 2 * HALO)
    parts[...] = jnp.zeros_like(parts)
    put_products(acc, parts, DD)


def far_residual_kernel(across, *refs):
    other, parts_d, refs = refs[: S + 1], refs[S + 1], refs[S + 2 :]
    chain, sums, sideways, acc, parts = refs[S : 2 * S], refs[2 * S], refs[2 * S + 1], refs[2 * S + 2], refs[2 * S + 3]
    rows = across.shape[2]
    load_planes(chain, across, range(HALO - 1, HALO - 1 - across.shape[0], -1))
    run_groups(far_groups(S - 1), chain, sideways, rows, S - 1)
    add_products(acc, chain, S - 1, other, rows - 2 * HALO)
    parts[...] = parts_d[...]
    put_products(acc, parts, RR)
    sums[...] = jnp.sum(parts[...].T, axis=0, keepdims=True)


def coefficients(sums):
    tall = 24
    shape = (tall, 128)
    i = lax.broadcasted_iota(jnp.int32, shape, 0)
    j = lax.broadcasted_iota(jnp.int32, shape, 1)
    row_r, col_r = i > S, j > S
    a = jnp.where(row_r, i - (S + 1), i)
    b = jnp.where(col_r, j - (S + 1), j)
    valid = jnp.logical_and(i < COLS, j < COLS)
    base = jnp.where(row_r, jnp.where(col_r, RR, DR), jnp.where(col_r, DR, DD))
    at_plus = jnp.where(valid, base + a + b, -1)
    at_minus = jnp.where(valid, base + jnp.abs(a - b), -1)
    at_base = jnp.where(valid, base + ((a + b) & 1), -1)
    gram = jnp.zeros(shape, jnp.float32)
    for place in range(SUMS):
        weight = (
            (at_plus == place).astype(jnp.float32)
            + (at_minus == place).astype(jnp.float32)
            - (at_base == place).astype(jnp.float32)
        )
        gram = gram + weight * sums[:, place : place + 1]

    def change(index, axis):
        second = index > S
        k = jnp.where(second, index - (S + 1), index)
        count = jnp.where(second, S, S + 1)
        valid = index < COLS
        middle = jnp.where(jnp.logical_and(valid, k < count - 1), 6.0, 0.0)
        below = jnp.where(jnp.logical_and(valid, k >= 1), jnp.where(k == 1, 6.0, 3.0), 0.0)
        above = jnp.where(jnp.logical_and(valid, k + 1 < count - 1), 3.0, 0.0)
        size = shape[axis]

        def apply(v):
            return middle * v + below * pltpu.roll(v, 1, axis) + above * pltpu.roll(v, size - 1, axis)

        return apply

    down, along = change(i, 0), change(j, 1)

    def quadratic(left_down, right_along):
        total = left_down * (gram * right_along)
        total = total[:8] + total[8:16] + total[16:]
        return jnp.sum(jnp.sum(total, axis=0, keepdims=True), axis=1, keepdims=True)

    def unit(index, k):
        return (index == k).astype(jnp.float32)

    q_d, q_a = unit(i, 0), unit(j, 0)
    w_d, w_a = unit(i, S + 1), unit(j, S + 1)
    c_d = jnp.zeros(shape, jnp.float32)
    rho = quadratic(w_d, w_a)
    for _ in range(S):
        m_d, m_a = down(q_d), along(q_a)
        alpha = rho / quadratic(q_d, m_a)
        c_d = c_d + alpha * q_d
        w_d, w_a = w_d - alpha * m_d, w_a - alpha * m_a
        rho_new = quadratic(w_d, w_a)
        beta = rho_new / rho
        q_d, q_a = w_d + beta * q_d, w_a + beta * q_a
        rho = rho_new
    return c_d, w_d, q_d


def combine(k, coefs, chain_d, chain_r, out, hold):
    per, keep = out.shape[1], out.shape[2]
    core, _ = here()
    first = per * piece_of(k)
    tile = 16

    def body(step, _):
        plane, at = step // (keep // tile), step % (keep // tile)
        row = pl.multiple_of(at * tile, tile)
        source = pl.ds(pl.multiple_of(PAD + HALO + row, 8), tile)
        where = HALO + jnp.where(core == 0, first + plane, PLANES - 1 - first - plane)
        sums = [[None] * 3, [None] * 3]
        for column in range(COLS):
            chain, power, steps = (chain_d, column, S) if column <= S else (chain_r, column - S - 1, S - 1)
            low = chain_plan(steps)[0][power]
            factors = [coefs[which, column : column + 1, :] for which in range(3)]
            for h in range(2):
                v = chain[power][where - low, h, source]
                for which in range(3):
                    term = v * factors[which]
                    sums[h][which] = term if column == 0 else sums[h][which] + term
        for h in range(2):
            for which in range(3):
                to = pl.multiple_of((which * per + plane) * keep + row, tile)
                hold[pl.ds(to, tile), h * HALF : (h + 1) * HALF] = sums[h][which]
        return 0

    lax.fori_loop(0, per * (keep // tile), body, 0)
    out[...] = move_columns(hold[...], parting(True)).reshape(out.shape)


def first_combine_kernel(k, sums, *refs):
    chain_d, chain_r, out, coefs, hold = refs[: S + 1], refs[S + 1 : COLS], *refs[COLS:]
    total = jnp.sum(sums[...], axis=0, keepdims=True)
    for which, value in enumerate(coefficients(total)):
        coefs[which] = value
    combine(k, coefs, chain_d, chain_r, out, hold)


def combine_kernel(k, coefs, *refs):
    combine(k, coefs, refs[: S + 1], refs[S + 1 : COLS], *refs[COLS:])


def finish_kernel(solution, *refs):
    pieces, outs, hold, sem = refs[:PIECES], refs[PIECES : PIECES + 3], refs[PIECES + 3], refs[PIECES + 4]
    _, per, keep, _ = pieces[0].shape
    copies = []
    for which in (1, 2, 0):
        for k in range(PIECES):
            rows = pl.ds(pl.multiple_of(piece_of(PIECES - k) * keep, keep), keep)
            for plane in range(per):
                value = pieces[k][which, plane]
                if which == 0:
                    value = value + solution[plane, rows]
                hold[which, plane, rows] = value
        copies.append(pltpu.make_async_copy(hold.at[which], outs[which], sem.at[which]))
        copies[-1].start()
    for copy in copies:
        copy.wait()


def on_device(solution, residual, direction):
    groups = lax.axis_size("x")
    outer = lax.axis_size("zz")
    per, height, lanes = direction.shape
    keep = height // groups
    rows = keep + 2 * HALO
    f32 = jnp.float32

    blocks = 2 * outer
    near = [(b, b - 1) for b in range(0, blocks, 2) if b > 0] + [(b, b + 1) for b in range(1, blocks, 2) if b + 1 < blocks]

    def params(mib=4):
        return pltpu.CompilerParams(vmem_limit_bytes=mib * 2**20)

    def cost(us):
        return pl.CostEstimate(flops=us * 10**7, bytes_accessed=0, transcendentals=0)

    def ahead(value, k):
        return lax.ppermute(value, "x", [(i, (i + k) % groups) for i in range(groups)])

    piece = jax.ShapeDtypeStruct((per, 2, rows, HALF), f32)

    def pack(field, name):
        keeps = [jax.ShapeDtypeStruct((per, 2, height, HALF), f32)] if name == "r" else []
        scratch = [] if name == "r" else [pltpu.VMEM((per, 2, height, HALF), f32)]
        return pl.pallas_call(
            pack_kernel,
            out_shape=[piece] * groups + keeps,
            in_specs=[VMEM],
            out_specs=[VMEM] * (groups + len(keeps)),
            scratch_shapes=scratch,
            compiler_params=params(),
            name="pack",
        )(field)

    def spread(pieces, mirrored=False):
        got = [pieces[0]]
        for k in range(1, groups):
            got.append(ahead(pieces[k], k))
        return pl.pallas_call(
            functools.partial(join_kernel, mirrored),
            out_shape=jax.ShapeDtypeStruct((PLANES, 2, rows, HALF), f32),
            in_specs=[VMEM] * groups,
            out_specs=VMEM,
            compiler_params=params(1),
            name="join",
        )(*got)

    def beside(own):
        return lax.ppermute(own, "c", [(0, 1), (1, 0)])

    def beyond(value):
        return lax.ppermute(value, ("zz", "c"), near)

    def chain_shapes(steps):
        return tuple(
            jax.ShapeDtypeStruct((end - low, 2, rows + 2 * PAD, HALF), f32) for low, end in zip(*chain_plan(steps))
        )

    sideways = pltpu.VMEM((GROUP, 2, rows, HALF), f32)

    def near_chain(steps, own, side):
        return pl.pallas_call(
            functools.partial(near_kernel, steps),
            out_shape=chain_shapes(steps),
            in_specs=[VMEM] * 2,
            out_specs=(VMEM,) * (steps + 1),
            scratch_shapes=[sideways],
            compiler_params=params(),
            cost_estimate=cost(4),
            name="near_chain",
        )(own, side)

    own_d = spread(pack(direction, "d"))
    side_d, across_d = beside(own_d), beyond(own_d)
    *pieces_r, parted_r = pack(residual, "r")
    far_r = beyond(parted_r)
    own_r = spread(pieces_r)
    side_r = beside(own_r)
    pieces_f = pl.pallas_call(
        cut_kernel,
        out_shape=[piece] * groups,
        in_specs=[VMEM],
        out_specs=[VMEM] * groups,
        compiler_params=params(1),
        name="cut",
    )(far_r)
    across_r = spread(pieces_f, mirrored=True)
    chain_d = near_chain(S, own_d, side_d)
    *chain_d, parts = pl.pallas_call(
        far_direction_kernel,
        out_shape=(*chain_shapes(S), jax.ShapeDtypeStruct((128, 128), f32)),
        in_specs=[VMEM] * (S + 2),
        out_specs=(VMEM,) * (S + 2),
        scratch_shapes=[sideways, pltpu.VMEM((2 * S + 1, 8, HALF), f32)],
        input_output_aliases={1 + k: k for k in range(S + 1)},
        compiler_params=params(),
        cost_estimate=cost(4),
        name="far_direction",
    )(across_d, *chain_d)
    chain_r = near_chain(S - 1, own_r, side_r)
    *chain_r, sums = pl.pallas_call(
        far_residual_kernel,
        out_shape=(*chain_shapes(S - 1), jax.ShapeDtypeStruct((1, 128), f32)),
        in_specs=[VMEM] * (2 * S + 3),
        out_specs=(VMEM,) * (S + 1),
        scratch_shapes=[sideways, pltpu.VMEM((4 * S - 1, 8, HALF), f32), pltpu.VMEM((128, 128), f32)],
        input_output_aliases={S + 3 + k: k for k in range(S)},
        compiler_params=params(),
        cost_estimate=cost(4),
        name="far_residual",
    )(across_r, *chain_d, parts, *chain_r)

    devices = groups * blocks
    everyone = lax.all_to_all(jnp.broadcast_to(sums[None], (devices, 1, 128)), ALL, 0, 0, tiled=True)

    mixed_shape = jax.ShapeDtypeStruct((3, per, keep, lanes), f32)
    hold = pltpu.VMEM((3 * per * keep, lanes), f32)
    mixed = {}
    first, *others = (2, 1, 3, 0)
    mixed[first], coefs = pl.pallas_call(
        functools.partial(first_combine_kernel, first),
        out_shape=(mixed_shape, jax.ShapeDtypeStruct((3, 24, 128), f32)),
        in_specs=[VMEM] * (COLS + 1),
        out_specs=(VMEM, VMEM),
        scratch_shapes=[hold],
        compiler_params=params(),
        cost_estimate=cost(4),
        name="combine",
    )(everyone.reshape(devices, 128), *chain_d, *chain_r)
    for k in others:
        mixed[k] = pl.pallas_call(
            functools.partial(combine_kernel, k),
            out_shape=mixed_shape,
            in_specs=[VMEM] * (COLS + 1),
            out_specs=VMEM,
            scratch_shapes=[hold],
            compiler_params=params(),
            cost_estimate=cost(1),
            name="combine",
        )(coefs, *chain_d, *chain_r)
    back = [mixed[0]]
    for k in range(1, groups):
        back.append(ahead(mixed[k], k))

    whole = jax.ShapeDtypeStruct((per, height, lanes), f32)
    return pl.pallas_call(
        finish_kernel,
        out_shape=(whole,) * 3,
        in_specs=[VMEM] * (groups + 1),
        out_specs=(HBM,) * 3,
        scratch_shapes=[pltpu.VMEM((3, per, height, lanes), f32), pltpu.SemaphoreType.DMA((3,))],
        compiler_params=params(8),
        name="finish",
    )(solution, *back)


def solution(mesh):
    blocks, groups = mesh.devices.shape
    split = Mesh(mesh.devices.reshape(blocks // 2, 2, groups), ALL)
    spec = P(ALL, None, None)

    return jax.shard_map(
        on_device, mesh=split, in_specs=(spec, spec, spec), out_specs=(spec, spec, spec), check_vma=False
    )
```

```python
import functools

import jax
import jax.numpy as jnp
from jax import lax
from jax.experimental import pallas as pl
from jax.experimental.pallas import tpu as pltpu
from jax.sharding import Mesh, PartitionSpec as P


S = 8
PIECES = 4
COLS = 2 * S + 1
PLANES = 8
HALO = 8
TALL = PLANES + 2 * HALO
PAD = 8
HALF = 128
GROUP = 4
BLOCK = 16
AHEAD = 4
FIRST = -1.0 / 6.0
NEXT = -1.0 / 3.0
ALL = ("zz", "c", "x")
VMEM = pl.BlockSpec(memory_space=pltpu.VMEM)
HBM = pl.BlockSpec(memory_space=pltpu.HBM)

DD, RR, DR = 0, 2 * S + 1, 4 * S
SUMS = 6 * S


def here():
    return lax.axis_index("c"), lax.axis_index("x")


def piece_of(k):
    return (lax.axis_index("x") + k) % PIECES


def chain_plan(steps):
    lows = [0] + [HALO - steps + k for k in range(1, steps + 1)]
    ends = [TALL] + [HALO + PLANES + steps - k for k in range(1, steps + 1)]
    return lows, ends


def parting(back):
    i = lax.broadcasted_iota(jnp.int32, (2 * HALF, 2 * HALF), 0 if back else 1)
    j = lax.broadcasted_iota(jnp.int32, (2 * HALF, 2 * HALF), 1 if back else 0)
    return (j == jnp.where(i < HALF, 2 * i, 2 * (i - HALF) + 1)).astype(jnp.bfloat16)


def move_columns(value, matrix):
    total = None
    for _ in range(3):
        part = value.astype(jnp.bfloat16)
        moved = jnp.dot(part, matrix, preferred_element_type=jnp.float32)
        total = moved if total is None else total + moved
        value = value - part.astype(jnp.float32)
    return total


def part_columns(source, out):
    matrix = parting(False)
    for plane in range(source.shape[0]):
        parted = move_columns(source[plane], matrix)
        for h in range(2):
            out[plane, h] = parted[:, h * HALF : (h + 1) * HALF]


def pack_kernel(source, *refs):
    part_columns(source, refs[PIECES])
    cut_kernel(refs[PIECES], *refs[:PIECES])


def cut_kernel(planes, *outs):
    per, halves, rows, _ = outs[0].shape
    keep, height = rows - 2 * HALO, planes.shape[2]
    for k in range(PIECES):
        g = piece_of(k)
        row = pl.multiple_of(g * keep, keep)
        below = pl.multiple_of(jnp.maximum(row - HALO, 0), HALO)
        above = pl.multiple_of(jnp.minimum(row + keep, height - HALO), HALO)
        has_below, has_above = (g != 0).astype(jnp.float32), (g != PIECES - 1).astype(jnp.float32)
        for plane in range(per):
            for h in range(halves):
                outs[k][plane, h, :HALO] = planes[plane, h, pl.ds(below, HALO)] * has_below
                outs[k][plane, h, pl.ds(HALO, keep)] = planes[plane, h, pl.ds(row, keep)]
                outs[k][plane, h, rows - HALO :] = planes[plane, h, pl.ds(above, HALO)] * has_above


def join_kernel(mirrored, *refs):
    out = refs[PIECES]
    core, _ = here()
    core = 1 - core if mirrored else core
    per = refs[0].shape[0]
    for k in range(PIECES):
        plane = per * piece_of(PIECES - k)
        for p in range(per):
            out[jnp.where(core == 0, plane + p, PLANES - 1 - plane - p)] = refs[k][p]


def load_planes(chain, source, places):
    rows = pl.ds(PAD, source.shape[2])
    for i, place in enumerate(places):
        for h in range(2):
            chain[0][place, h, rows] = source[i, h]


def run_groups(groups, chain, rows, steps):
    lows, _ = chain_plan(steps)
    core, x = here()
    zz = lax.axis_index("zz")
    last = lax.axis_size("zz") - 1
    alone = jnp.logical_or(jnp.logical_and(zz == 0, core == 0), jnp.logical_and(zz == last, core == 1))
    low_x = (x != 0).astype(jnp.float32)
    high_x = (x != PIECES - 1).astype(jnp.float32)
    across_valid = 1.0 - alone.astype(jnp.float32)
    lane = lax.broadcasted_iota(jnp.int32, (BLOCK, HALF), 1)
    at_low, at_high = lane == 0, lane == HALF - 1
    blocks = rows // BLOCK
    items = [(power, plane, count, block) for power, plane, count in groups for block in range(blocks)]
    missing = {(power, plane + u, block) for power, plane, count, block in items for u in range(count)}

    def read(power, plane, h, block, shift=0):
        return chain[power][plane - lows[power], h, pl.ds(PAD + BLOCK * block + shift, BLOCK)]

    def rotate(power, plane, count, block):
        turned = []
        for u in range(count):
            a, b = (read(power - 1, plane + u, h, block) for h in range(2))
            turned.append((pltpu.roll(b, 1, 1), pltpu.roll(a, HALF - 1, 1)))
        return turned

    def compute(power, plane, count, block, turned):
        near = [[read(power - 1, plane + u, h, block) for h in range(2)] for u in range(-1, count + 1)]
        for u in range(count):
            scale = FIRST if power == 1 else NEXT
            if plane + u < HALO:
                scale = scale * across_valid
            for h in range(2):
                beside = near[u + 1][1 - h] + jnp.where(at_high if h else at_low, 0.0, turned[u][h])
                total = near[u][h] + near[u + 2][h]
                total = total + (read(power - 1, plane + u, h, block, -1) + read(power - 1, plane + u, h, block, 1))
                total = total + beside
                if block == 0:
                    total = jnp.concatenate([total[:HALO] * (scale * low_x), total[HALO:] * scale], axis=0)
                elif block == blocks - 1:
                    total = jnp.concatenate([total[:-HALO] * scale, total[-HALO:] * (scale * high_x)], axis=0)
                else:
                    total = total * scale
                if power > 1:
                    total = total - read(power - 2, plane + u, h, block)
                chain[power][plane + u - lows[power], h, pl.ds(PAD + BLOCK * block, BLOCK)] = total
            missing.discard((power, plane + u, block))

    turned, pushed = {}, 0
    for i, item in enumerate(items):
        while pushed < min(len(items), i + 1 + AHEAD):
            power, plane, count, block = items[pushed]
            if any((power - 1, plane + u, block) in missing for u in range(count)):
                break
            turned[pushed] = rotate(*items[pushed])
            pushed += 1
        compute(*item, turned.pop(i))


def near_groups(steps):
    _, ends = chain_plan(steps)
    groups = []
    for power in range(1, steps + 1):
        low, end = HALO + power, ends[power]
        left = end - low
        while left > 0:
            count = min(GROUP, left)
            if left in (5, 6):
                count = 3
            groups.append((power, low, count))
            low, left = low + count, left - count
    return groups


def far_groups(steps):
    lows, _ = chain_plan(steps)
    groups = []
    for power in range(1, steps + 1):
        middle = HALO + power - GROUP
        groups.append((power, middle, GROUP))
        groups.append((power, lows[power], middle - lows[power]))
    return groups


def near_kernel(steps, own, side, *refs):
    chain = refs[: steps + 1]
    load_planes(chain, own, range(HALO, HALO + PLANES))
    load_planes(chain, side, range(TALL - 1, HALO + PLANES - 1, -1))
    run_groups(near_groups(steps), chain, own.shape[2], steps)


def add_products(acc, chain, steps, other, keep):
    _, _ = chain_plan(steps)
    rows = pl.ds(PAD + HALO, keep)
    acc[...] = jnp.zeros_like(acc)

    def total(a, b):
        return jnp.sum((a * b).reshape(keep // 8, 8, HALF), axis=0)

    def body(step, _):
        plane, h = step // 2, step % 2

        def of(chain, steps, k):
            return chain[k][HALO + plane - chain_plan(steps)[0][k], h, rows]

        before, beside = None, None
        if other:
            beside = of(other, S, 0)
        for k in range(steps + 1):
            now = of(chain, steps, k)
            acc[2 * k] += total(now, now)
            if k:
                acc[2 * k - 1] += total(before, now)
            if other:
                following = of(other, S, k + 1)
                acc[2 * steps + 1 + 2 * k] += total(beside, now)
                acc[2 * steps + 2 + 2 * k] += total(following, now)
                beside = following
            before = now
        return 0

    lax.fori_loop(0, 2 * PLANES, body, 0)


def put_products(acc, parts, place):
    for k in range(acc.shape[0]):
        parts[pl.ds(place + k, 1), :] = jnp.sum(acc[k], axis=0, keepdims=True)


def far_direction_kernel(across, *refs):
    chain, parts, acc = refs[S + 1 : 2 * S + 2], refs[2 * S + 2], refs[2 * S + 3]
    rows = across.shape[2]
    load_planes(chain, across, range(HALO - 1, HALO - 1 - across.shape[0], -1))
    run_groups(far_groups(S), chain, rows, S)
    add_products(acc, chain, S, None, rows - 2 * HALO)
    parts[...] = jnp.zeros_like(parts)
    put_products(acc, parts, DD)


def far_residual_kernel(across, *refs):
    other, parts_d, refs = refs[: S + 1], refs[S + 1], refs[S + 2 :]
    chain, sums, acc, parts = refs[S : 2 * S], refs[2 * S], refs[2 * S + 1], refs[2 * S + 2]
    rows = across.shape[2]
    load_planes(chain, across, range(HALO - 1, HALO - 1 - across.shape[0], -1))
    run_groups(far_groups(S - 1), chain, rows, S - 1)
    add_products(acc, chain, S - 1, other, rows - 2 * HALO)
    parts[...] = parts_d[...]
    put_products(acc, parts, RR)
    sums[...] = jnp.sum(parts[...].T, axis=0, keepdims=True)


def coefficients(sums):
    tall = 24
    shape = (tall, 128)
    i = lax.broadcasted_iota(jnp.int32, shape, 0)
    j = lax.broadcasted_iota(jnp.int32, shape, 1)
    row_r, col_r = i > S, j > S
    a = jnp.where(row_r, i - (S + 1), i)
    b = jnp.where(col_r, j - (S + 1), j)
    valid = jnp.logical_and(i < COLS, j < COLS)
    base = jnp.where(row_r, jnp.where(col_r, RR, DR), jnp.where(col_r, DR, DD))
    at_plus = jnp.where(valid, base + a + b, -1)
    at_minus = jnp.where(valid, base + jnp.abs(a - b), -1)
    at_base = jnp.where(valid, base + ((a + b) & 1), -1)
    gram = jnp.zeros(shape, jnp.float32)
    for place in range(SUMS):
        weight = (
            (at_plus == place).astype(jnp.float32)
            + (at_minus == place).astype(jnp.float32)
            - (at_base == place).astype(jnp.float32)
        )
        gram = gram + weight * sums[:, place : place + 1]

    def change(index, axis):
        second = index > S
        k = jnp.where(second, index - (S + 1), index)
        count = jnp.where(second, S, S + 1)
        valid = index < COLS
        middle = jnp.where(jnp.logical_and(valid, k < count - 1), 6.0, 0.0)
        below = jnp.where(jnp.logical_and(valid, k >= 1), jnp.where(k == 1, 6.0, 3.0), 0.0)
        above = jnp.where(jnp.logical_and(valid, k + 1 < count - 1), 3.0, 0.0)
        size = shape[axis]

        def apply(v):
            return middle * v + below * pltpu.roll(v, 1, axis) + above * pltpu.roll(v, size - 1, axis)

        return apply

    down, along = change(i, 0), change(j, 1)

    def quadratic(left_down, right_along):
        total = left_down * (gram * right_along)
        total = total[:8] + total[8:16] + total[16:]
        return jnp.sum(jnp.sum(total, axis=0, keepdims=True), axis=1, keepdims=True)

    def unit(index, k):
        return (index == k).astype(jnp.float32)

    q_d, q_a = unit(i, 0), unit(j, 0)
    w_d, w_a = unit(i, S + 1), unit(j, S + 1)
    c_d = jnp.zeros(shape, jnp.float32)
    rho = quadratic(w_d, w_a)
    for _ in range(S):
        m_d, m_a = down(q_d), along(q_a)
        alpha = rho / quadratic(q_d, m_a)
        c_d = c_d + alpha * q_d
        w_d, w_a = w_d - alpha * m_d, w_a - alpha * m_a
        rho_new = quadratic(w_d, w_a)
        beta = rho_new / rho
        q_d, q_a = w_d + beta * q_d, w_a + beta * q_a
        rho = rho_new
    return c_d, w_d, q_d


def combine(k, coefs, chain_d, chain_r, out, hold):
    per, keep = out.shape[1], out.shape[2]
    core, _ = here()
    first = per * piece_of(k)
    tile = 16

    def body(step, _):
        plane, at = step // (keep // tile), step % (keep // tile)
        row = pl.multiple_of(at * tile, tile)
        source = pl.ds(pl.multiple_of(PAD + HALO + row, 8), tile)
        where = HALO + jnp.where(core == 0, first + plane, PLANES - 1 - first - plane)
        sums = [[None] * 3, [None] * 3]
        for column in range(COLS):
            chain, power, steps = (chain_d, column, S) if column <= S else (chain_r, column - S - 1, S - 1)
            low = chain_plan(steps)[0][power]
            factors = [coefs[which, column : column + 1, :] for which in range(3)]
            for h in range(2):
                v = chain[power][where - low, h, source]
                for which in range(3):
                    term = v * factors[which]
                    sums[h][which] = term if column == 0 else sums[h][which] + term
        for h in range(2):
            for which in range(3):
                to = pl.multiple_of((which * per + plane) * keep + row, tile)
                hold[pl.ds(to, tile), h * HALF : (h + 1) * HALF] = sums[h][which]
        return 0

    lax.fori_loop(0, per * (keep // tile), body, 0)
    out[...] = move_columns(hold[...], parting(True)).reshape(out.shape)


def first_combine_kernel(k, sums, *refs):
    chain_d, chain_r, out, coefs, hold = refs[: S + 1], refs[S + 1 : COLS], *refs[COLS:]
    total = jnp.sum(sums[...], axis=0, keepdims=True)
    for which, value in enumerate(coefficients(total)):
        coefs[which] = value
    combine(k, coefs, chain_d, chain_r, out, hold)


def combine_kernel(k, coefs, *refs):
    combine(k, coefs, refs[: S + 1], refs[S + 1 : COLS], *refs[COLS:])


def finish_kernel(solution, *refs):
    pieces, outs, hold, sem = refs[:PIECES], refs[PIECES : PIECES + 3], refs[PIECES + 3], refs[PIECES + 4]
    _, per, keep, _ = pieces[0].shape
    copies = []
    for which in (1, 2, 0):
        for k in range(PIECES):
            rows = pl.ds(pl.multiple_of(piece_of(PIECES - k) * keep, keep), keep)
            for plane in range(per):
                value = pieces[k][which, plane]
                if which == 0:
                    value = value + solution[plane, rows]
                hold[which, plane, rows] = value
        copies.append(pltpu.make_async_copy(hold.at[which], outs[which], sem.at[which]))
        copies[-1].start()
    for copy in copies:
        copy.wait()


def on_device(solution, residual, direction):
    groups = lax.axis_size("x")
    outer = lax.axis_size("zz")
    per, height, lanes = direction.shape
    keep = height // groups
    rows = keep + 2 * HALO
    f32 = jnp.float32

    blocks = 2 * outer
    near = [(b, b - 1) for b in range(0, blocks, 2) if b > 0] + [(b, b + 1) for b in range(1, blocks, 2) if b + 1 < blocks]

    def params(mib=4):
        return pltpu.CompilerParams(vmem_limit_bytes=mib * 2**20)

    def cost(us):
        return pl.CostEstimate(flops=us * 10**7, bytes_accessed=0, transcendentals=0)

    def ahead(value, k):
        return lax.ppermute(value, "x", [(i, (i + k) % groups) for i in range(groups)])

    piece = jax.ShapeDtypeStruct((per, 2, rows, HALF), f32)

    def pack(field, name):
        keeps = [jax.ShapeDtypeStruct((per, 2, height, HALF), f32)] if name == "r" else []
        scratch = [] if name == "r" else [pltpu.VMEM((per, 2, height, HALF), f32)]
        return pl.pallas_call(
            pack_kernel,
            out_shape=[piece] * groups + keeps,
            in_specs=[VMEM],
            out_specs=[VMEM] * (groups + len(keeps)),
            scratch_shapes=scratch,
            compiler_params=params(),
            name="pack",
        )(field)

    def spread(pieces, mirrored=False):
        got = [pieces[0]]
        for k in range(1, groups):
            got.append(ahead(pieces[k], k))
        return pl.pallas_call(
            functools.partial(join_kernel, mirrored),
            out_shape=jax.ShapeDtypeStruct((PLANES, 2, rows, HALF), f32),
            in_specs=[VMEM] * groups,
            out_specs=VMEM,
            compiler_params=params(1),
            name="join",
        )(*got)

    def beside(own):
        return lax.ppermute(own, "c", [(0, 1), (1, 0)])

    def beyond(value):
        return lax.ppermute(value, ("zz", "c"), near)

    def chain_shapes(steps):
        return tuple(
            jax.ShapeDtypeStruct((end - low, 2, rows + 2 * PAD, HALF), f32) for low, end in zip(*chain_plan(steps))
        )

    def near_chain(steps, own, side):
        return pl.pallas_call(
            functools.partial(near_kernel, steps),
            out_shape=chain_shapes(steps),
            in_specs=[VMEM] * 2,
            out_specs=(VMEM,) * (steps + 1),
            compiler_params=params(),
            cost_estimate=cost(4),
            name="near_chain",
        )(own, side)

    own_d = spread(pack(direction, "d"))
    side_d, across_d = beside(own_d), beyond(own_d)
    *pieces_r, parted_r = pack(residual, "r")
    far_r = beyond(parted_r)
    own_r = spread(pieces_r)
    side_r = beside(own_r)
    pieces_f = pl.pallas_call(
        cut_kernel,
        out_shape=[piece] * groups,
        in_specs=[VMEM],
        out_specs=[VMEM] * groups,
        compiler_params=params(1),
        name="cut",
    )(far_r)
    across_r = spread(pieces_f, mirrored=True)
    chain_d = near_chain(S, own_d, side_d)
    *chain_d, parts = pl.pallas_call(
        far_direction_kernel,
        out_shape=(*chain_shapes(S), jax.ShapeDtypeStruct((128, 128), f32)),
        in_specs=[VMEM] * (S + 2),
        out_specs=(VMEM,) * (S + 2),
        scratch_shapes=[pltpu.VMEM((2 * S + 1, 8, HALF), f32)],
        input_output_aliases={1 + k: k for k in range(S + 1)},
        compiler_params=params(),
        cost_estimate=cost(4),
        name="far_direction",
    )(across_d, *chain_d)
    chain_r = near_chain(S - 1, own_r, side_r)
    *chain_r, sums = pl.pallas_call(
        far_residual_kernel,
        out_shape=(*chain_shapes(S - 1), jax.ShapeDtypeStruct((1, 128), f32)),
        in_specs=[VMEM] * (2 * S + 3),
        out_specs=(VMEM,) * (S + 1),
        scratch_shapes=[pltpu.VMEM((4 * S - 1, 8, HALF), f32), pltpu.VMEM((128, 128), f32)],
        input_output_aliases={S + 3 + k: k for k in range(S)},
        compiler_params=params(),
        cost_estimate=cost(4),
        name="far_residual",
    )(across_r, *chain_d, parts, *chain_r)

    devices = groups * blocks
    everyone = lax.all_to_all(jnp.broadcast_to(sums[None], (devices, 1, 128)), ALL, 0, 0, tiled=True)

    mixed_shape = jax.ShapeDtypeStruct((3, per, keep, lanes), f32)
    hold = pltpu.VMEM((3 * per * keep, lanes), f32)
    mixed = {}
    first, *others = (2, 1, 3, 0)
    mixed[first], coefs = pl.pallas_call(
        functools.partial(first_combine_kernel, first),
        out_shape=(mixed_shape, jax.ShapeDtypeStruct((3, 24, 128), f32)),
        in_specs=[VMEM] * (COLS + 1),
        out_specs=(VMEM, VMEM),
        scratch_shapes=[hold],
        compiler_params=params(),
        cost_estimate=cost(4),
        name="combine",
    )(everyone.reshape(devices, 128), *chain_d, *chain_r)
    for k in others:
        mixed[k] = pl.pallas_call(
            functools.partial(combine_kernel, k),
            out_shape=mixed_shape,
            in_specs=[VMEM] * (COLS + 1),
            out_specs=VMEM,
            scratch_shapes=[hold],
            compiler_params=params(),
            cost_estimate=cost(1),
            name="combine",
        )(coefs, *chain_d, *chain_r)
    back = [mixed[0]]
    for k in range(1, groups):
        back.append(ahead(mixed[k], k))

    whole = jax.ShapeDtypeStruct((per, height, lanes), f32)
    return pl.pallas_call(
        finish_kernel,
        out_shape=(whole,) * 3,
        in_specs=[VMEM] * (groups + 1),
        out_specs=(HBM,) * 3,
        scratch_shapes=[pltpu.VMEM((3, per, height, lanes), f32), pltpu.SemaphoreType.DMA((3,))],
        compiler_params=params(8),
        name="finish",
    )(solution, *back)


def solution(mesh):
    blocks, groups = mesh.devices.shape
    split = Mesh(mesh.devices.reshape(blocks // 2, 2, groups), ALL)
    spec = P(ALL, None, None)

    return jax.shard_map(
        on_device, mesh=split, in_specs=(spec, spec, spec), out_specs=(spec, spec, spec), check_vma=False
    )
```

```python
import functools

import jax
import jax.numpy as jnp
from jax import lax
from jax.experimental import pallas as pl
from jax.experimental.pallas import tpu as pltpu
from jax.sharding import Mesh, PartitionSpec as P


S = 8
PIECES = 4
COLS = 2 * S + 1
PLANES = 8
HALO = 8
TALL = PLANES + 2 * HALO
PAD = 8
HALF = 128
GROUP = 4
BLOCK = 16
AHEAD = 4
FIRST = -1.0 / 6.0
NEXT = -1.0 / 3.0
ALL = ("zz", "c", "x")
VMEM = pl.BlockSpec(memory_space=pltpu.VMEM)
HBM = pl.BlockSpec(memory_space=pltpu.HBM)

DD, RR, DR = 0, 2 * S + 1, 4 * S
SUMS = 6 * S


def here():
    return lax.axis_index("c"), lax.axis_index("x")


def piece_of(k):
    return (lax.axis_index("x") + k) % PIECES


def chain_plan(steps):
    lows = [0] + [HALO - steps + k for k in range(1, steps + 1)]
    ends = [TALL] + [HALO + PLANES + steps - k for k in range(1, steps + 1)]
    return lows, ends


def parting(back):
    i = lax.broadcasted_iota(jnp.int32, (2 * HALF, 2 * HALF), 0 if back else 1)
    j = lax.broadcasted_iota(jnp.int32, (2 * HALF, 2 * HALF), 1 if back else 0)
    return (j == jnp.where(i < HALF, 2 * i, 2 * (i - HALF) + 1)).astype(jnp.bfloat16)


def move_columns(value, matrix):
    total = None
    for _ in range(3):
        part = value.astype(jnp.bfloat16)
        moved = jnp.dot(part, matrix, preferred_element_type=jnp.float32)
        total = moved if total is None else total + moved
        value = value - part.astype(jnp.float32)
    return total


def part_columns(source, out):
    matrix = parting(False)
    for plane in range(source.shape[0]):
        parted = move_columns(source[plane], matrix)
        for h in range(2):
            out[plane, h] = parted[:, h * HALF : (h + 1) * HALF]


def pack_kernel(source, *refs):
    part_columns(source, refs[PIECES])
    cut_kernel(refs[PIECES], *refs[:PIECES])


def first_pack_kernel(direction, residual, *refs):
    outs, fetched, stage, parted, sem = refs[:PIECES], *refs[PIECES:]
    copies = [
        pltpu.make_async_copy(source.at[plane], to.at[plane], sem.at[2 * field + plane])
        for field, (source, to) in enumerate(((direction, stage), (residual, fetched)))
        for plane in range(direction.shape[0])
    ]
    for copy in copies:
        copy.start()
    for copy in copies[:2]:
        copy.wait()
    part_columns(stage, parted)
    cut_kernel(parted, *outs)
    for copy in copies[2:]:
        copy.wait()


def cut_kernel(planes, *outs):
    per, halves, rows, _ = outs[0].shape
    keep, height = rows - 2 * HALO, planes.shape[2]
    for k in range(PIECES):
        g = piece_of(k)
        row = pl.multiple_of(g * keep, keep)
        below = pl.multiple_of(jnp.maximum(row - HALO, 0), HALO)
        above = pl.multiple_of(jnp.minimum(row + keep, height - HALO), HALO)
        has_below, has_above = (g != 0).astype(jnp.float32), (g != PIECES - 1).astype(jnp.float32)
        for plane in range(per):
            for h in range(halves):
                outs[k][plane, h, :HALO] = planes[plane, h, pl.ds(below, HALO)] * has_below
                outs[k][plane, h, pl.ds(HALO, keep)] = planes[plane, h, pl.ds(row, keep)]
                outs[k][plane, h, rows - HALO :] = planes[plane, h, pl.ds(above, HALO)] * has_above


def join_kernel(mirrored, *refs):
    out = refs[PIECES]
    core, _ = here()
    core = 1 - core if mirrored else core
    per = refs[0].shape[0]
    for k in range(PIECES):
        plane = per * piece_of(PIECES - k)
        for p in range(per):
            out[jnp.where(core == 0, plane + p, PLANES - 1 - plane - p)] = refs[k][p]


def load_planes(chain, source, places):
    rows = pl.ds(PAD, source.shape[2])
    for i, place in enumerate(places):
        for h in range(2):
            chain[0][place, h, rows] = source[i, h]


def run_groups(groups, chain, rows, steps):
    lows, _ = chain_plan(steps)
    core, x = here()
    zz = lax.axis_index("zz")
    last = lax.axis_size("zz") - 1
    alone = jnp.logical_or(jnp.logical_and(zz == 0, core == 0), jnp.logical_and(zz == last, core == 1))
    low_x = (x != 0).astype(jnp.float32)
    high_x = (x != PIECES - 1).astype(jnp.float32)
    across_valid = 1.0 - alone.astype(jnp.float32)
    lane = lax.broadcasted_iota(jnp.int32, (BLOCK, HALF), 1)
    at_low, at_high = lane == 0, lane == HALF - 1
    blocks = rows // BLOCK
    items = [(power, plane, count, block) for power, plane, count in groups for block in range(blocks)]
    missing = {(power, plane + u, block) for power, plane, count, block in items for u in range(count)}

    def read(power, plane, h, block, shift=0):
        return chain[power][plane - lows[power], h, pl.ds(PAD + BLOCK * block + shift, BLOCK)]

    def rotate(power, plane, count, block):
        turned = []
        for u in range(count):
            a, b = (read(power - 1, plane + u, h, block) for h in range(2))
            turned.append((pltpu.roll(b, 1, 1), pltpu.roll(a, HALF - 1, 1)))
        return turned

    def compute(power, plane, count, block, turned):
        near = [[read(power - 1, plane + u, h, block) for h in range(2)] for u in range(-1, count + 1)]
        for u in range(count):
            scale = FIRST if power == 1 else NEXT
            if plane + u < HALO:
                scale = scale * across_valid
            for h in range(2):
                beside = near[u + 1][1 - h] + jnp.where(at_high if h else at_low, 0.0, turned[u][h])
                total = near[u][h] + near[u + 2][h]
                total = total + (read(power - 1, plane + u, h, block, -1) + read(power - 1, plane + u, h, block, 1))
                total = total + beside
                if block == 0:
                    total = jnp.concatenate([total[:HALO] * (scale * low_x), total[HALO:] * scale], axis=0)
                elif block == blocks - 1:
                    total = jnp.concatenate([total[:-HALO] * scale, total[-HALO:] * (scale * high_x)], axis=0)
                else:
                    total = total * scale
                if power > 1:
                    total = total - read(power - 2, plane + u, h, block)
                chain[power][plane + u - lows[power], h, pl.ds(PAD + BLOCK * block, BLOCK)] = total
            missing.discard((power, plane + u, block))

    turned, pushed = {}, 0
    for i, item in enumerate(items):
        while pushed < min(len(items), i + 1 + AHEAD):
            power, plane, count, block = items[pushed]
            if any((power - 1, plane + u, block) in missing for u in range(count)):
                break
            turned[pushed] = rotate(*items[pushed])
            pushed += 1
        compute(*item, turned.pop(i))


def near_groups(steps):
    _, ends = chain_plan(steps)
    groups = []
    for power in range(1, steps + 1):
        low, end = HALO + power, ends[power]
        left = end - low
        while left > 0:
            count = min(GROUP, left)
            if left in (5, 6):
                count = 3
            groups.append((power, low, count))
            low, left = low + count, left - count
    return groups


def far_groups(steps):
    lows, _ = chain_plan(steps)
    groups = []
    for power in range(1, steps + 1):
        middle = HALO + power - GROUP
        groups.append((power, middle, GROUP))
        groups.append((power, lows[power], middle - lows[power]))
    return groups


def near_kernel(steps, own, side, *refs):
    chain = refs[: steps + 1]
    load_planes(chain, own, range(HALO, HALO + PLANES))
    load_planes(chain, side, range(TALL - 1, HALO + PLANES - 1, -1))
    run_groups(near_groups(steps), chain, own.shape[2], steps)


def add_products(acc, chain, steps, other, keep):
    _, _ = chain_plan(steps)
    rows = pl.ds(PAD + HALO, keep)
    acc[...] = jnp.zeros_like(acc)

    def total(a, b):
        return jnp.sum((a * b).reshape(keep // 8, 8, HALF), axis=0)

    def body(step, _):
        plane, h = step // 2, step % 2

        def of(chain, steps, k):
            return chain[k][HALO + plane - chain_plan(steps)[0][k], h, rows]

        before, beside = None, None
        if other:
            beside = of(other, S, 0)
        for k in range(steps + 1):
            now = of(chain, steps, k)
            acc[2 * k] += total(now, now)
            if k:
                acc[2 * k - 1] += total(before, now)
            if other:
                following = of(other, S, k + 1)
                acc[2 * steps + 1 + 2 * k] += total(beside, now)
                acc[2 * steps + 2 + 2 * k] += total(following, now)
                beside = following
            before = now
        return 0

    lax.fori_loop(0, 2 * PLANES, body, 0)


def put_products(acc, parts, place):
    for k in range(acc.shape[0]):
        parts[pl.ds(place + k, 1), :] = jnp.sum(acc[k], axis=0, keepdims=True)


def far_direction_kernel(across, *refs):
    chain, parts, acc = refs[S + 1 : 2 * S + 2], refs[2 * S + 2], refs[2 * S + 3]
    rows = across.shape[2]
    load_planes(chain, across, range(HALO - 1, HALO - 1 - across.shape[0], -1))
    run_groups(far_groups(S), chain, rows, S)
    add_products(acc, chain, S, None, rows - 2 * HALO)
    parts[...] = jnp.zeros_like(parts)
    put_products(acc, parts, DD)


def far_residual_kernel(across, *refs):
    other, parts_d, refs = refs[: S + 1], refs[S + 1], refs[S + 2 :]
    chain, sums, acc, parts = refs[S : 2 * S], refs[2 * S], refs[2 * S + 1], refs[2 * S + 2]
    rows = across.shape[2]
    load_planes(chain, across, range(HALO - 1, HALO - 1 - across.shape[0], -1))
    run_groups(far_groups(S - 1), chain, rows, S - 1)
    add_products(acc, chain, S - 1, other, rows - 2 * HALO)
    parts[...] = parts_d[...]
    put_products(acc, parts, RR)
    sums[...] = jnp.sum(parts[...].T, axis=0, keepdims=True)


def coefficients(sums):
    tall = 24
    shape = (tall, 128)
    i = lax.broadcasted_iota(jnp.int32, shape, 0)
    j = lax.broadcasted_iota(jnp.int32, shape, 1)
    row_r, col_r = i > S, j > S
    a = jnp.where(row_r, i - (S + 1), i)
    b = jnp.where(col_r, j - (S + 1), j)
    valid = jnp.logical_and(i < COLS, j < COLS)
    base = jnp.where(row_r, jnp.where(col_r, RR, DR), jnp.where(col_r, DR, DD))
    at_plus = jnp.where(valid, base + a + b, -1)
    at_minus = jnp.where(valid, base + jnp.abs(a - b), -1)
    at_base = jnp.where(valid, base + ((a + b) & 1), -1)
    gram = jnp.zeros(shape, jnp.float32)
    for place in range(SUMS):
        weight = (
            (at_plus == place).astype(jnp.float32)
            + (at_minus == place).astype(jnp.float32)
            - (at_base == place).astype(jnp.float32)
        )
        gram = gram + weight * sums[:, place : place + 1]

    def change(index, axis):
        second = index > S
        k = jnp.where(second, index - (S + 1), index)
        count = jnp.where(second, S, S + 1)
        valid = index < COLS
        middle = jnp.where(jnp.logical_and(valid, k < count - 1), 6.0, 0.0)
        below = jnp.where(jnp.logical_and(valid, k >= 1), jnp.where(k == 1, 6.0, 3.0), 0.0)
        above = jnp.where(jnp.logical_and(valid, k + 1 < count - 1), 3.0, 0.0)
        size = shape[axis]

        def apply(v):
            return middle * v + below * pltpu.roll(v, 1, axis) + above * pltpu.roll(v, size - 1, axis)

        return apply

    down, along = change(i, 0), change(j, 1)

    def quadratic(left_down, right_along):
        total = left_down * (gram * right_along)
        total = total[:8] + total[8:16] + total[16:]
        return jnp.sum(jnp.sum(total, axis=0, keepdims=True), axis=1, keepdims=True)

    def unit(index, k):
        return (index == k).astype(jnp.float32)

    q_d, q_a = unit(i, 0), unit(j, 0)
    w_d, w_a = unit(i, S + 1), unit(j, S + 1)
    c_d = jnp.zeros(shape, jnp.float32)
    rho = quadratic(w_d, w_a)
    for _ in range(S):
        m_d, m_a = down(q_d), along(q_a)
        alpha = rho / quadratic(q_d, m_a)
        c_d = c_d + alpha * q_d
        w_d, w_a = w_d - alpha * m_d, w_a - alpha * m_a
        rho_new = quadratic(w_d, w_a)
        beta = rho_new / rho
        q_d, q_a = w_d + beta * q_d, w_a + beta * q_a
        rho = rho_new
    return c_d, w_d, q_d


def combine(k, coefs, chain_d, chain_r, out, hold):
    per, keep = out.shape[1], out.shape[2]
    core, _ = here()
    first = per * piece_of(k)
    tile = 16

    def body(step, _):
        plane, at = step // (keep // tile), step % (keep // tile)
        row = pl.multiple_of(at * tile, tile)
        source = pl.ds(pl.multiple_of(PAD + HALO + row, 8), tile)
        where = HALO + jnp.where(core == 0, first + plane, PLANES - 1 - first - plane)
        sums = [[None] * 3, [None] * 3]
        for column in range(COLS):
            chain, power, steps = (chain_d, column, S) if column <= S else (chain_r, column - S - 1, S - 1)
            low = chain_plan(steps)[0][power]
            factors = [coefs[which, column : column + 1, :] for which in range(3)]
            for h in range(2):
                v = chain[power][where - low, h, source]
                for which in range(3):
                    term = v * factors[which]
                    sums[h][which] = term if column == 0 else sums[h][which] + term
        for h in range(2):
            for which in range(3):
                to = pl.multiple_of((which * per + plane) * keep + row, tile)
                hold[pl.ds(to, tile), h * HALF : (h + 1) * HALF] = sums[h][which]
        return 0

    lax.fori_loop(0, per * (keep // tile), body, 0)
    out[...] = move_columns(hold[...], parting(True)).reshape(out.shape)


def first_combine_kernel(k, sums, *refs):
    chain_d, chain_r, out, coefs, hold = refs[: S + 1], refs[S + 1 : COLS], *refs[COLS:]
    total = jnp.sum(sums[...], axis=0, keepdims=True)
    for which, value in enumerate(coefficients(total)):
        coefs[which] = value
    combine(k, coefs, chain_d, chain_r, out, hold)


def combine_kernel(k, coefs, *refs):
    combine(k, coefs, refs[: S + 1], refs[S + 1 : COLS], *refs[COLS:])


def finish_kernel(solution, *refs):
    pieces, outs, hold, sem = refs[:PIECES], refs[PIECES : PIECES + 3], refs[PIECES + 3], refs[PIECES + 4]
    _, per, keep, _ = pieces[0].shape
    copies = []
    for which in (1, 2, 0):
        for k in range(PIECES):
            rows = pl.ds(pl.multiple_of(piece_of(PIECES - k) * keep, keep), keep)
            for plane in range(per):
                value = pieces[k][which, plane]
                if which == 0:
                    value = value + solution[plane, rows]
                hold[which, plane, rows] = value
        copies.append(pltpu.make_async_copy(hold.at[which], outs[which], sem.at[which]))
        copies[-1].start()
    for copy in copies:
        copy.wait()


def on_device(solution, residual, direction):
    groups = lax.axis_size("x")
    outer = lax.axis_size("zz")
    per, height, lanes = direction.shape
    keep = height // groups
    rows = keep + 2 * HALO
    f32 = jnp.float32

    blocks = 2 * outer
    near = [(b, b - 1) for b in range(0, blocks, 2) if b > 0] + [(b, b + 1) for b in range(1, blocks, 2) if b + 1 < blocks]

    def params(mib=4):
        return pltpu.CompilerParams(vmem_limit_bytes=mib * 2**20)

    def cost(us):
        return pl.CostEstimate(flops=us * 10**7, bytes_accessed=0, transcendentals=0)

    def ahead(value, k):
        return lax.ppermute(value, "x", [(i, (i + k) % groups) for i in range(groups)])

    piece = jax.ShapeDtypeStruct((per, 2, rows, HALF), f32)

    parted = jax.ShapeDtypeStruct((per, 2, height, HALF), f32)
    whole = jax.ShapeDtypeStruct((per, height, lanes), f32)
    *pieces_d, fetched = pl.pallas_call(
        first_pack_kernel,
        out_shape=[piece] * groups + [whole],
        in_specs=[HBM] * 2,
        out_specs=[VMEM] * (groups + 1),
        scratch_shapes=[
            pltpu.VMEM(whole.shape, f32),
            pltpu.VMEM(parted.shape, f32),
            pltpu.SemaphoreType.DMA((2 * per,)),
        ],
        compiler_params=params(),
        name="pack",
    )(*(pltpu.with_memory_space_constraint(field, pltpu.HBM) for field in (direction, residual)))
    *pieces_r, parted_r = pl.pallas_call(
        pack_kernel,
        out_shape=[piece] * groups + [parted],
        in_specs=[VMEM],
        out_specs=[VMEM] * (groups + 1),
        compiler_params=params(),
        name="pack",
    )(fetched)

    def spread(pieces, mirrored=False):
        got = [pieces[0]]
        for k in range(1, groups):
            got.append(ahead(pieces[k], k))
        return pl.pallas_call(
            functools.partial(join_kernel, mirrored),
            out_shape=jax.ShapeDtypeStruct((PLANES, 2, rows, HALF), f32),
            in_specs=[VMEM] * groups,
            out_specs=VMEM,
            compiler_params=params(1),
            name="join",
        )(*got)

    def beside(own):
        return lax.ppermute(own, "c", [(0, 1), (1, 0)])

    def beyond(value):
        return lax.ppermute(value, ("zz", "c"), near)

    def chain_shapes(steps):
        return tuple(
            jax.ShapeDtypeStruct((end - low, 2, rows + 2 * PAD, HALF), f32) for low, end in zip(*chain_plan(steps))
        )

    def near_chain(steps, own, side):
        return pl.pallas_call(
            functools.partial(near_kernel, steps),
            out_shape=chain_shapes(steps),
            in_specs=[VMEM] * 2,
            out_specs=(VMEM,) * (steps + 1),
            compiler_params=params(),
            cost_estimate=cost(4),
            name="near_chain",
        )(own, side)

    own_d = spread(pieces_d)
    side_d, across_d = beside(own_d), beyond(own_d)
    far_r = beyond(parted_r)
    own_r = spread(pieces_r)
    side_r = beside(own_r)
    pieces_f = pl.pallas_call(
        cut_kernel,
        out_shape=[piece] * groups,
        in_specs=[VMEM],
        out_specs=[VMEM] * groups,
        compiler_params=params(1),
        name="cut",
    )(far_r)
    across_r = spread(pieces_f, mirrored=True)
    chain_d = near_chain(S, own_d, side_d)
    *chain_d, parts = pl.pallas_call(
        far_direction_kernel,
        out_shape=(*chain_shapes(S), jax.ShapeDtypeStruct((128, 128), f32)),
        in_specs=[VMEM] * (S + 2),
        out_specs=(VMEM,) * (S + 2),
        scratch_shapes=[pltpu.VMEM((2 * S + 1, 8, HALF), f32)],
        input_output_aliases={1 + k: k for k in range(S + 1)},
        compiler_params=params(),
        cost_estimate=cost(4),
        name="far_direction",
    )(across_d, *chain_d)
    chain_r = near_chain(S - 1, own_r, side_r)
    *chain_r, sums = pl.pallas_call(
        far_residual_kernel,
        out_shape=(*chain_shapes(S - 1), jax.ShapeDtypeStruct((1, 128), f32)),
        in_specs=[VMEM] * (2 * S + 3),
        out_specs=(VMEM,) * (S + 1),
        scratch_shapes=[pltpu.VMEM((4 * S - 1, 8, HALF), f32), pltpu.VMEM((128, 128), f32)],
        input_output_aliases={S + 3 + k: k for k in range(S)},
        compiler_params=params(),
        cost_estimate=cost(4),
        name="far_residual",
    )(across_r, *chain_d, parts, *chain_r)

    devices = groups * blocks
    everyone = lax.all_to_all(jnp.broadcast_to(sums[None], (devices, 1, 128)), ALL, 0, 0, tiled=True)

    mixed_shape = jax.ShapeDtypeStruct((3, per, keep, lanes), f32)
    hold = pltpu.VMEM((3 * per * keep, lanes), f32)
    mixed = {}
    first, *others = (2, 1, 3, 0)
    mixed[first], coefs = pl.pallas_call(
        functools.partial(first_combine_kernel, first),
        out_shape=(mixed_shape, jax.ShapeDtypeStruct((3, 24, 128), f32)),
        in_specs=[VMEM] * (COLS + 1),
        out_specs=(VMEM, VMEM),
        scratch_shapes=[hold],
        compiler_params=params(),
        cost_estimate=cost(4),
        name="combine",
    )(everyone.reshape(devices, 128), *chain_d, *chain_r)
    for k in others:
        mixed[k] = pl.pallas_call(
            functools.partial(combine_kernel, k),
            out_shape=mixed_shape,
            in_specs=[VMEM] * (COLS + 1),
            out_specs=VMEM,
            scratch_shapes=[hold],
            compiler_params=params(),
            cost_estimate=cost(1),
            name="combine",
        )(coefs, *chain_d, *chain_r)
    back = [mixed[0]]
    for k in range(1, groups):
        back.append(ahead(mixed[k], k))

    return pl.pallas_call(
        finish_kernel,
        out_shape=(whole,) * 3,
        in_specs=[VMEM] * (groups + 1),
        out_specs=(HBM,) * 3,
        scratch_shapes=[pltpu.VMEM((3, per, height, lanes), f32), pltpu.SemaphoreType.DMA((3,))],
        compiler_params=params(8),
        name="finish",
    )(solution, *back)


def solution(mesh):
    blocks, groups = mesh.devices.shape
    split = Mesh(mesh.devices.reshape(blocks // 2, 2, groups), ALL)
    spec = P(ALL, None, None)

    return jax.shard_map(
        on_device, mesh=split, in_specs=(spec, spec, spec), out_specs=(spec, spec, spec), check_vma=False
    )
```
